32 devices in a mesh: row: 8 (over y, x, core), col: 4 (over z).
Axes of the slice: x: 2, y: 2, z: 4, core: 2. Of those that a mesh axis runs over, the one named last changes fastest.
Arguments:
- residual: float32 [2048, 2048], P('row', 'col'), may hold values from -0.15625 to 0.15625
- direction: float32 [2048, 2048], P('row', 'col'), may hold values from -6 to 6
- ground_shift: float32 [1], replicated, may hold values from 1.6937256e-06 to 6.7749024e-06
- previous: float32 [1], replicated, may hold values from 192 to 768
Outputs:
- next_direction: float32 [2048, 2048], P('row', 'col')
- step_ratio: float32 [1], replicated
The draws below stay inside these ranges and needn't reach their ends.
All inputs are finite; a program needn't handle non-finite values.
Results may differ from the reference program's by a relative error of at most 0.00015.
Values sent between devices are 32-bit elements; how exact they have to be, the bound alone decides.
A program may use at most 64 MiB of HBM per device.

```python
import math
import jax
import jax.numpy as jnp
from jax import lax

Q0 = 256
NX = 2048
NY = 2048


def draw_residual(key, part):
    subkeys = jax.random.split(jax.random.fold_in(key, 17), 2)
    row_place = jnp.arange(NX, dtype=jnp.int32).astype(jnp.float32) / NX
    col_scale = jnp.exp(jax.random.uniform(subkeys[1], (NY,), jnp.float32, 0.0, jnp.log(10.0)))
    base_scale = 0.1 / Q0
    row_scale = jnp.exp(row_place * jnp.log(10.0))
    samples = jnp.clip(jax.random.normal(subkeys[0], (NX, NY), jnp.float32), -4.0, 4.0)
    return base_scale * row_scale[:, None] * col_scale[None, :] * samples


def shard_levels(key, dims, cuts, low, largest):
    level = 1.0
    for axis_at, blocks in cuts:
        steps = jax.random.uniform(jax.random.fold_in(jax.random.fold_in(key, 6), axis_at), (blocks,), jnp.float32, low / len(cuts), largest / len(cuts))
        level = level * jnp.repeat(jnp.exp(steps), dims[axis_at] // blocks).reshape((-1,) + (1,) * (len(dims) - 1 - axis_at))
    return level


def gaussian(rng, dims, scale, reach, pieces=(), held_as=jnp.bfloat16):
    result = jax.random.normal(rng, dims, jnp.float32) * scale
    if len(pieces) > 0:
        result = shard_levels(rng, dims, pieces, -0.22, 0.18) * result
    return jnp.clip(result, min=-reach, max=reach).astype(held_as)


def setup_inputs(seed: int = 0) -> dict:
    streams_of = jax.random.split(jax.random.key(seed), 5)
    residual = draw_residual(jax.random.fold_in(streams_of[4], 71), 0)
    direction = gaussian(streams_of[1], (NX, NY), 1.0, 6.0, ((0, 8), (1, 4)), jnp.float32)
    ground_shift = jnp.clip(jnp.exp(jax.random.uniform(streams_of[2], (1,), jnp.float32, math.log(1.6937256077653728e-06), math.log(6.774902431061491e-06))), 1.6937256077653728e-06, 6.774902431061491e-06)
    previous = jnp.clip(jnp.exp(jax.random.uniform(streams_of[3], (1,), jnp.float32, math.log(192.0), math.log(768.0))), 192.0, 768.0)
    return dict(residual=residual, direction=direction, ground_shift=ground_shift, previous=previous)


PRECISE = lax.Precision.HIGHEST

def cosine_matrix(length):
    wavenum = jnp.arange(length, dtype=jnp.int32)[:, None]
    position = jnp.arange(length, dtype=jnp.int32)[None, :]
    phases = wavenum * (2 * position + 1) % (4 * length)
    angles = jnp.pi * phases.astype(jnp.float32) / (2 * length)
    scaling = jnp.where(wavenum == 0, jnp.sqrt(1.0 / length), jnp.sqrt(2.0 / length)).astype(jnp.float32)
    return scaling * jnp.cos(angles)

def reference(residual, direction, ground_shift, previous):
    rows_table = cosine_matrix(NX)
    cols_table = cosine_matrix(NY)
    spectrum = jnp.dot(jnp.dot(rows_table, residual, precision=PRECISE), cols_table.T, precision=PRECISE)
    row_waves = jnp.arange(NX, dtype=jnp.int32).astype(jnp.float32)
    col_waves = jnp.arange(NY, dtype=jnp.int32).astype(jnp.float32)
    row_sine = jnp.sin(jnp.pi * row_waves / (2 * NX))
    col_sine = jnp.sin(jnp.pi * col_waves / (2 * NY))
    eigenvalue = 4.0 * (row_sine * row_sine)[:, None] + 4.0 * (col_sine * col_sine)[None, :]
    weight = 1.0 / (eigenvalue + ground_shift[0])
    scaled = weight * spectrum
    precond = jnp.dot(jnp.dot(rows_table.T, scaled, precision=PRECISE), cols_table, precision=PRECISE)
    inner_total = jnp.sum(residual * precond)
    step_ratio = inner_total / previous[0]
    return (precond + step_ratio * direction, jnp.reshape(step_ratio, (1,)))
```

```python
import functools
import math

import jax
import jax.numpy as jnp
import numpy as np
from jax import lax
from jax.experimental import pallas as pl
from jax.experimental.pallas import tpu as pltpu
from jax.sharding import PartitionSpec as P

MESH = pl.DeviceIdType.MESH


def base_tables(extent, devices):
    length = extent * devices
    half = extent // 2
    odd = 2 * np.arange(extent, dtype=np.int64)[:, None] + 1
    steps = 2 * devices * np.arange(half + 1, dtype=np.int64)[None, :]
    coarse = np.pi * (steps * odd % (4 * length)) / (2 * length)
    scale = math.sqrt(2.0 / length)
    cos_a, sin_a = scale * np.cos(coarse), scale * np.sin(coarse)
    lanes = -(-(devices + 1) // 128) * 128
    fine = np.pi * np.arange(lanes, dtype=np.int64)[None, :] * odd / (2 * length)
    coarse_tables = np.stack([cos_a[:, :-1], sin_a[:, :-1], cos_a[:, 1:], sin_a[:, 1:]])
    fine_tables = np.stack([np.cos(fine), np.sin(fine)])
    waves = []
    for t in range(devices):
        second = devices if t == 0 else 2 * devices - t
        waves.append(2 * devices * np.arange(half) + t)
        waves.append(2 * devices * np.arange(half) + second)
    waves = np.concatenate(waves)
    eigen = 4.0 * np.sin(np.pi * waves / (2 * length)) ** 2
    return (
        coarse_tables.astype(np.float32),
        fine_tables.astype(np.float32),
        eigen.astype(np.float32)[None, :],
    )


def mixing(devices):
    target = np.arange(devices)[:, None]
    source = np.arange(devices)[None, :]
    angles = np.pi * (target * source % (2 * devices)) / devices
    parity = np.where(source % 2 == 0, 1.0, -1.0)
    return np.cos(angles), np.where(target > 0, np.sin(angles), parity)


def weighted_sum(coefs, terms):
    total = None
    for coef, term in zip(coefs, terms):
        coef = float(coef)
        if abs(coef) < 1e-12:
            continue
        if abs(coef - 1.0) < 1e-12:
            total = term if total is None else total + term
        elif abs(coef + 1.0) < 1e-12:
            total = -term if total is None else total - term
        else:
            total = coef * term if total is None else total + coef * term
    return total


def split(value):
    high = value.astype(jnp.bfloat16)
    return high, (value - high.astype(jnp.float32)).astype(jnp.bfloat16)


def kernel(
    rows,
    cols,
    residual_hbm,
    coarse_hbm,
    fine_hbm,
    eigen_hbm,
    shift_hbm,
    previous_hbm,
    out_ref,
    ratio_ref,
    residual_ref,
    coarse_ref,
    fine_ref,
    eigen_ref,
    shift_ref,
    previous_ref,
    load_sems,
    out1,
    in1,
    out2,
    in2,
    table_hi,
    table_lo,
    field,
    from_left,
    from_right,
    own_hi,
    own_lo,
    carried_hi,
    carried_lo,
    added,
    rowsum,
    colsum,
    carry,
    s1,
    r1,
    s2,
    r2,
    s3,
    r3,
    s5,
    r5,
):
    me_r = lax.axis_index("row")
    me_c = lax.axis_index("col")
    extent = residual_ref.shape[0]
    width = out1.shape[1]
    half = extent // 2
    total_cols = width * rows * cols
    f32 = jnp.float32
    mix_cos, mix_sin = mixing(rows)

    barrier = pltpu.get_barrier_semaphore()
    for o in range(1, rows):
        pl.semaphore_signal(
            barrier, inc=1, device_id={"row": lax.rem(me_r + o, rows)}, device_id_type=MESH
        )
    for o in range(1, cols):
        pl.semaphore_signal(
            barrier, inc=1, device_id={"col": lax.rem(me_c + o, cols)}, device_id_type=MESH
        )

    loads = []
    for i, (source, landing) in enumerate(
        (
            (residual_hbm, residual_ref),
            (coarse_hbm, coarse_ref),
            (fine_hbm, fine_ref),
            (eigen_hbm, eigen_ref),
            (shift_hbm, shift_ref),
            (previous_hbm, previous_ref),
        )
    ):
        copy = pltpu.make_async_copy(source, landing, load_sems.at[i])
        copy.start()
        loads.append(copy)

    def share(axis, me, count, source, landing, send_sems, recv_sems):
        copies = []
        for o in range(1, count):
            to = lax.rem(me + o, count)
            copy = pltpu.make_async_remote_copy(
                src_ref=source(to),
                dst_ref=landing.at[me],
                send_sem=send_sems.at[o - 1],
                recv_sem=recv_sems.at[o - 1],
                device_id={axis: to},
                device_id_type=MESH,
            )
            copy.start()
            copies.append(copy)
        return copies

    loads[0].wait()
    for e in range(0, residual_ref.shape[1], 128):
        turned = residual_ref[:, e : e + 128].T
        for i in range(128 // width):
            out1[e // width + i] = turned[i * width : (i + 1) * width]
    pl.semaphore_wait(barrier, rows + cols - 2)
    first = share("row", me_r, rows, lambda to: out1.at[to], in1, s1, r1)
    in1[me_r] = out1[me_r]

    loads[1].wait()
    loads[2].wait()

    def quadrants(t):
        if t == 0:
            lane = lax.broadcasted_iota(jnp.int32, (extent, half), 1)
            one = jnp.where(lane == 0, math.sqrt(0.5), 1.0) * coarse_ref[0]
            cos_b = fine_ref[0, :, rows : rows + 1]
            sin_b = fine_ref[1, :, rows : rows + 1]
            two = coarse_ref[0] * cos_b - coarse_ref[1] * sin_b
            zero = jnp.zeros_like(one)
            return ((one, zero), (zero, two))
        cos_b = fine_ref[0, :, t : t + 1]
        sin_b = fine_ref[1, :, t : t + 1]
        return (
            (
                coarse_ref[0] * cos_b - coarse_ref[1] * sin_b,
                coarse_ref[2] * cos_b + coarse_ref[3] * sin_b,
            ),
            (
                -(coarse_ref[1] * cos_b + coarse_ref[0] * sin_b),
                coarse_ref[3] * cos_b - coarse_ref[2] * sin_b,
            ),
        )

    for t in range(rows):
        quads = quadrants(t)
        for i in range(2):
            for j in range(2):
                high, low = split(quads[i][j])
                at = (t, slice(i * extent, (i + 1) * extent), slice(j * half, (j + 1) * half))
                table_hi[at] = high
                table_lo[at] = low

    for copy in loads[3:]:
        copy.wait()
    alpha = eigen_ref[...] + shift_ref[0]
    h = 0.5 * jnp.sqrt(alpha)
    z = h / (1.0 + jnp.sqrt(1.0 + h * h))
    z2 = z * z
    series = jnp.full_like(z, 1.0 / 23)
    for p in range(21, 0, -2):
        series = series * z2 + 1.0 / p
    theta = 4.0 * z * series
    gain = 0.5 / jnp.sqrt(alpha * (1.0 + 0.25 * alpha))

    q_one = jnp.exp(-theta)
    place = lax.broadcasted_iota(jnp.int32, (width, extent), 0)
    fplace = place.astype(f32)
    for t in range(rows):
        lanes = slice(t * extent, (t + 1) * extent)
        from_left[:, lanes] = gain[:, lanes] * jnp.exp(-theta[:, lanes] * (fplace + 1.0))
        from_right[:, lanes] = gain[:, lanes] * jnp.exp(-theta[:, lanes] * (width - fplace))
    chunk = jnp.exp(-theta * float(width))
    group = jnp.exp(-theta * float(width * rows))
    whole = jnp.exp(-theta * float(total_cols))

    for copy in first:
        copy.wait_recv()

    length = rows * extent
    partial = jnp.zeros((1, extent), f32)
    for t in range(rows):
        lanes = slice(t * extent, (t + 1) * extent)
        pieces = [in1[d] for d in range(rows)]
        real = weighted_sum(mix_cos[t], pieces)
        imag = weighted_sum(mix_sin[t], pieces)
        high, low = split(jnp.concatenate([real, imag], axis=1))
        both = jnp.dot(
            jnp.concatenate([high, low], axis=0), table_hi[t], preferred_element_type=f32
        )
        value = (
            both[:width] + both[width:] + jnp.dot(high, table_lo[t], preferred_element_type=f32)
        )
        ahead = value
        behind = value
        q = q_one[:, lanes]
        s = 1
        while s < width:
            ahead = ahead + q * jnp.where(place >= s, pltpu.roll(ahead, s, 0), 0.0)
            behind = behind + q * jnp.where(
                place < width - s, pltpu.roll(behind, width - s, 0), 0.0
            )
            q = q * q
            s *= 2
        solved = gain[:, lanes] * (ahead + behind - value)
        partial = partial + jnp.sum(value * solved, axis=0, keepdims=True)
        field[:, lanes] = solved
        rowsum[me_r, 0:1, lanes] = ahead[width - 1 : width]
        rowsum[me_r, 1:2, lanes] = behind[0:1]

    def fold(row):
        return sum(row[:, i : i + 128] for i in range(0, row.shape[1], 128))

    spare = slice(length, length + 128)
    rowsum[me_r, 0:1, spare] = fold(partial)
    rowsum[me_r, 1:2, spare] = jnp.zeros((1, 128), f32)
    mine = rowsum.at[me_r]
    second = share("row", me_r, rows, lambda to: mine, rowsum, s2, r2)

    turn = (((1,), (1,)), ((), ()))
    reals, imags = [], []
    for t in range(rows):
        lanes = slice(t * extent, (t + 1) * extent)
        high, low = split(field[:, lanes])
        both = lax.dot_general(
            jnp.concatenate([high, low], axis=0), table_hi[t], turn, preferred_element_type=f32
        )
        value = (
            both[:width]
            + both[width:]
            + lax.dot_general(high, table_lo[t], turn, preferred_element_type=f32)
        )
        reals.append(value[:, :extent])
        imags.append(value[:, extent:])
    for d in range(rows):
        out2[d] = weighted_sum(list(mix_cos[:, d]) + list(mix_sin[:, d]), reals + imags)
    fifth = share("row", me_r, rows, lambda to: out2.at[to], in2, s5, r5)
    in2[me_r] = out2[me_r]
    for copy in second:
        copy.wait_recv()

    def carries(sums, count, ratio):
        left, right = [jnp.zeros_like(ratio)], [jnp.zeros_like(ratio)]
        for k in range(count):
            left.append(ratio * left[-1] + sums[k, 0:1, :length])
            right.append(ratio * right[-1] + sums[count - 1 - k, 1:2, :length])
        return left[:-1], right[count - 1 :: -1], left[-1], right[-1]

    weight = gain * q_one
    lefts, rights, at_end, at_start = carries(rowsum, rows, chunk)
    coupled = jnp.zeros_like(weight)
    inner = jnp.zeros((1, 128), f32)
    for k in range(rows):
        carry[k, 0:1, :] = lefts[k]
        carry[k, 1:2, :] = rights[k]
        coupled = coupled + lefts[k] * rowsum[k, 1:2, :length] + rights[k] * rowsum[k, 0:1, :length]
        inner = inner + rowsum[k, 0:1, spare]
    colsum[me_c, 0:1, :length] = at_end
    colsum[me_c, 1:2, :length] = at_start
    colsum[me_c, 0:1, spare] = inner + fold(weight * coupled)
    colsum[me_c, 1:2, spare] = jnp.zeros((1, 128), f32)
    mine_c = colsum.at[me_c]
    third = share("col", me_c, cols, lambda to: mine_c, colsum, s3, r3)

    for t in range(rows):
        quads = quadrants(t)
        cos_d, sin_d = f32(mix_cos[t, 0]), f32(mix_sin[t, 0])
        for d in range(1, rows):
            cos_d = jnp.where(me_r == d, f32(mix_cos[t, d]), cos_d)
            sin_d = jnp.where(me_r == d, f32(mix_sin[t, d]), sin_d)
        for j in range(2):
            high, low = split(cos_d * quads[0][j] + sin_d * quads[1][j])
            lanes = slice(t * extent + j * half, t * extent + (j + 1) * half)
            own_hi[:, lanes] = high
            own_lo[:, lanes] = low
    for copy in third:
        copy.wait_recv()

    lefts, rights, at_end, at_start = carries(colsum, cols, group)
    images = 1.0 / (1.0 - whole * whole)
    entry = (at_start + whole * at_end) * images
    exit_ = (at_end + whole * at_start) * images
    for k in range(cols):
        lefts[k] = lefts[k] + entry
        rights[cols - 1 - k] = rights[cols - 1 - k] + exit_
        entry, exit_ = entry * group, exit_ * group
    coupled = jnp.zeros_like(weight)
    inner = jnp.zeros((1, 128), f32)
    left_c, right_c = lefts[0], rights[0]
    for k in range(cols):
        left_c = jnp.where(me_c == k, lefts[k], left_c)
        right_c = jnp.where(me_c == k, rights[k], right_c)
        coupled = coupled + lefts[k] * colsum[k, 1:2, :length] + rights[k] * colsum[k, 0:1, :length]
        inner = inner + colsum[k, 0:1, spare]
    inner = jnp.sum(inner + fold(weight * coupled), axis=1, keepdims=True)
    ratio = inner / previous_ref[0]
    ratio_ref[...] = jnp.broadcast_to(ratio, ratio_ref.shape)
    for k in range(rows):
        carry[k, 0:1, :] = carry[k, 0:1, :] + left_c
        carry[rows - 1 - k, 1:2, :] = carry[rows - 1 - k, 1:2, :] + right_c
        left_c, right_c = left_c * chunk, right_c * chunk

    per = 128 // width
    block = out_ref.shape[1]
    for e in range(0, out_ref.shape[1], block):
        for r in range(e // width, (e + block) // width):
            at = slice(r * width, (r + 1) * width)
            for t in range(rows):
                lanes = slice(t * extent, (t + 1) * extent)
                high, low = split(
                    from_left[:, lanes] * carry[r, 0:1, lanes]
                    + from_right[:, lanes] * carry[r, 1:2, lanes]
                )
                carried_hi[at, lanes] = high
                carried_lo[at, lanes] = low
        at = slice(e, e + block)
        added[at, :] = (
            lax.dot_general(carried_hi[at, :], own_hi[...], turn, preferred_element_type=f32)
            + lax.dot_general(carried_lo[at, :], own_hi[...], turn, preferred_element_type=f32)
            + lax.dot_general(carried_hi[at, :], own_lo[...], turn, preferred_element_type=f32)
        )
    for copy in fifth:
        copy.wait_recv()
    for e in range(0, out_ref.shape[1], 128):
        turned = jnp.concatenate([in2[e // width + i] for i in range(per)], axis=0)
        turned = turned + added[e : e + 128, :]
        out_ref[:, e : e + 128] = turned.T
    for copies in (first, second, third, fifth):
        for copy in copies:
            copy.wait_send()


def body(rows, cols, residual, direction, ground_shift, previous):
    extent, here = residual.shape
    width = here // rows
    length = extent * rows
    f32 = jnp.float32
    coarse, fine, eigen = base_tables(extent, rows)
    vmem = pl.BlockSpec(memory_space=pltpu.VMEM)
    smem = pl.BlockSpec(memory_space=pltpu.SMEM)
    dma = pltpu.SemaphoreType.DMA
    per_row, per_col = max(rows - 1, 1), max(cols - 1, 1)
    hbm = pl.BlockSpec(memory_space=pltpu.HBM)
    scratch = [
        pltpu.VMEM((extent, here), f32),
        pltpu.VMEM(coarse.shape, f32),
        pltpu.VMEM(fine.shape, f32),
        pltpu.VMEM(eigen.shape, f32),
        pltpu.SMEM((1,), f32),
        pltpu.SMEM((1,), f32),
        dma((6,)),
        pltpu.VMEM((rows, width, extent), f32),
        pltpu.VMEM((rows, width, extent), f32),
        pltpu.VMEM((rows, width, extent), f32),
        pltpu.VMEM((rows, width, extent), f32),
        pltpu.VMEM((rows, 2 * extent, extent), jnp.bfloat16),
        pltpu.VMEM((rows, 2 * extent, extent), jnp.bfloat16),
        pltpu.VMEM((width, length), f32),
        pltpu.VMEM((width, length), f32),
        pltpu.VMEM((width, length), f32),
        pltpu.VMEM((extent, length), jnp.bfloat16),
        pltpu.VMEM((extent, length), jnp.bfloat16),
        pltpu.VMEM((here, length), jnp.bfloat16),
        pltpu.VMEM((here, length), jnp.bfloat16),
        pltpu.VMEM((here, extent), f32),
        pltpu.VMEM((rows, 2, length + 128), f32),
        pltpu.VMEM((cols, 2, length + 128), f32),
        pltpu.VMEM((rows, 2, length), f32),
        dma((per_row,)),
        dma((per_row,)),
        dma((per_row,)),
        dma((per_row,)),
        dma((per_col,)),
        dma((per_col,)),
        dma((per_row,)),
        dma((per_row,)),
    ]
    held = sum(
        math.prod(ref.shape) * jnp.dtype(ref.dtype).itemsize
        for ref in scratch
        if ref.memory_space == pltpu.VMEM
    )
    solved, ratio = pl.pallas_call(
        functools.partial(kernel, rows, cols),
        out_shape=(
            jax.ShapeDtypeStruct((extent, here), f32),
            jax.ShapeDtypeStruct((1, 128), f32),
        ),
        in_specs=[hbm] * 6,
        out_specs=(vmem, vmem),
        scratch_shapes=scratch,
        compiler_params=pltpu.CompilerParams(
            collective_id=0, has_side_effects=True, vmem_limit_bytes=min(held + (held >> 2) + (4 << 20), 60 << 20)
        ),
    )(residual, coarse, fine, eigen, ground_shift, previous)
    return pl.pallas_call(
        update,
        out_shape=(
            jax.ShapeDtypeStruct((extent, here), f32),
            jax.ShapeDtypeStruct((1,), f32),
        ),
        in_specs=[vmem, vmem, vmem],
        out_specs=(vmem, smem),
        compiler_params=pltpu.CompilerParams(vmem_limit_bytes=8 * 1024 * 1024),
    )(solved, direction, ratio)


def update(solved_ref, direction_ref, ratio_in, out_ref, ratio_out):
    ratio = ratio_in[0:1, 0:1]
    out_ref[...] = solved_ref[...] + ratio * direction_ref[...]
    ratio_out[0] = ratio_in[0, 0]


def solution(mesh):
    return jax.shard_map(
        functools.partial(body, mesh.shape["row"], mesh.shape["col"]),
        mesh=mesh,
        in_specs=(P("row", "col"), P("row", "col"), P(), P()),
        out_specs=(P("row", "col"), P()),
        check_vma=False,
    )
```

```python
import functools
import math

import jax
import jax.numpy as jnp
import numpy as np
from jax import lax
from jax.experimental import pallas as pl
from jax.experimental.pallas import tpu as pltpu
from jax.sharding import PartitionSpec as P

MESH = pl.DeviceIdType.MESH


def base_tables(extent, devices):
    length = extent * devices
    half = extent // 2
    odd = 2 * np.arange(extent, dtype=np.int64)[:, None] + 1
    steps = 2 * devices * np.arange(half + 1, dtype=np.int64)[None, :]
    coarse = np.pi * (steps * odd % (4 * length)) / (2 * length)
    scale = math.sqrt(2.0 / length)
    cos_a, sin_a = scale * np.cos(coarse), scale * np.sin(coarse)
    lanes = -(-(devices + 1) // 128) * 128
    fine = np.pi * np.arange(lanes, dtype=np.int64)[None, :] * odd / (2 * length)
    coarse_tables = np.stack([cos_a[:, :-1], sin_a[:, :-1], cos_a[:, 1:], sin_a[:, 1:]])
    fine_tables = np.stack([np.cos(fine), np.sin(fine)])
    waves = []
    for t in range(devices):
        second = devices if t == 0 else 2 * devices - t
        waves.append(2 * devices * np.arange(half) + t)
        waves.append(2 * devices * np.arange(half) + second)
    waves = np.concatenate(waves)
    eigen = 4.0 * np.sin(np.pi * waves / (2 * length)) ** 2
    return (
        coarse_tables.astype(np.float32),
        fine_tables.astype(np.float32),
        eigen.astype(np.float32)[None, :],
    )


def mixing(devices):
    target = np.arange(devices)[:, None]
    source = np.arange(devices)[None, :]
    angles = np.pi * (target * source % (2 * devices)) / devices
    parity = np.where(source % 2 == 0, 1.0, -1.0)
    return np.cos(angles), np.where(target > 0, np.sin(angles), parity)


def weighted_sum(coefs, terms):
    total = None
    for coef, term in zip(coefs, terms):
        coef = float(coef)
        if abs(coef) < 1e-12:
            continue
        if abs(coef - 1.0) < 1e-12:
            total = term if total is None else total + term
        elif abs(coef + 1.0) < 1e-12:
            total = -term if total is None else total - term
        else:
            total = coef * term if total is None else total + coef * term
    return total


def split(value):
    high = value.astype(jnp.bfloat16)
    return high, (value - high.astype(jnp.float32)).astype(jnp.bfloat16)


def kernel(
    rows,
    cols,
    residual_hbm,
    coarse_hbm,
    fine_hbm,
    eigen_hbm,
    scalars_ref,
    out_ref,
    ratio_ref,
    residual_ref,
    coarse_ref,
    fine_ref,
    eigen_ref,
    load_sems,
    out1,
    in1,
    out2,
    in2,
    table_hi,
    table_lo,
    field,
    from_left,
    from_right,
    own_hi,
    own_lo,
    carried_hi,
    carried_lo,
    added,
    rowsum,
    colsum,
    carry,
    s1,
    r1,
    s2,
    r2,
    s3,
    r3,
    s5,
    r5,
):
    me_r = lax.axis_index("row")
    me_c = lax.axis_index("col")
    extent = residual_ref.shape[0]
    width = out1.shape[1]
    half = extent // 2
    total_cols = width * rows * cols
    f32 = jnp.float32
    mix_cos, mix_sin = mixing(rows)

    barrier = pltpu.get_barrier_semaphore()
    for o in range(1, rows):
        pl.semaphore_signal(
            barrier, inc=1, device_id={"row": lax.rem(me_r + o, rows)}, device_id_type=MESH
        )
    for o in range(1, cols):
        pl.semaphore_signal(
            barrier, inc=1, device_id={"col": lax.rem(me_c + o, cols)}, device_id_type=MESH
        )

    loads = []
    for i, (source, landing) in enumerate(
        (
            (residual_hbm, residual_ref),
            (coarse_hbm, coarse_ref),
            (fine_hbm, fine_ref),
            (eigen_hbm, eigen_ref),
        )
    ):
        copy = pltpu.make_async_copy(source, landing, load_sems.at[i])
        copy.start()
        loads.append(copy)

    def share(axis, me, count, source, landing, send_sems, recv_sems):
        copies = []
        for o in range(1, count):
            to = lax.rem(me + o, count)
            copy = pltpu.make_async_remote_copy(
                src_ref=source(to),
                dst_ref=landing.at[me],
                send_sem=send_sems.at[o - 1],
                recv_sem=recv_sems.at[o - 1],
                device_id={axis: to},
                device_id_type=MESH,
            )
            copy.start()
            copies.append(copy)
        return copies

    loads[0].wait()
    for e in range(0, residual_ref.shape[1], 128):
        turned = residual_ref[:, e : e + 128].T
        for i in range(128 // width):
            out1[e // width + i] = turned[i * width : (i + 1) * width]
    pl.semaphore_wait(barrier, rows + cols - 2)
    first = share("row", me_r, rows, lambda to: out1.at[to], in1, s1, r1)
    in1[me_r] = out1[me_r]

    loads[1].wait()
    loads[2].wait()

    def quadrants(t):
        if t == 0:
            lane = lax.broadcasted_iota(jnp.int32, (extent, half), 1)
            one = jnp.where(lane == 0, math.sqrt(0.5), 1.0) * coarse_ref[0]
            cos_b = fine_ref[0, :, rows : rows + 1]
            sin_b = fine_ref[1, :, rows : rows + 1]
            two = coarse_ref[0] * cos_b - coarse_ref[1] * sin_b
            zero = jnp.zeros_like(one)
            return ((one, zero), (zero, two))
        cos_b = fine_ref[0, :, t : t + 1]
        sin_b = fine_ref[1, :, t : t + 1]
        return (
            (
                coarse_ref[0] * cos_b - coarse_ref[1] * sin_b,
                coarse_ref[2] * cos_b + coarse_ref[3] * sin_b,
            ),
            (
                -(coarse_ref[1] * cos_b + coarse_ref[0] * sin_b),
                coarse_ref[3] * cos_b - coarse_ref[2] * sin_b,
            ),
        )

    for t in range(rows):
        quads = quadrants(t)
        for i in range(2):
            for j in range(2):
                high, low = split(quads[i][j])
                at = (t, slice(i * extent, (i + 1) * extent), slice(j * half, (j + 1) * half))
                table_hi[at] = high
                table_lo[at] = low

    for copy in loads[3:]:
        copy.wait()
    alpha = eigen_ref[...] + scalars_ref[0:1, 0:1]
    h = 0.5 * jnp.sqrt(alpha)
    z = h / (1.0 + jnp.sqrt(1.0 + h * h))
    z2 = z * z
    series = jnp.full_like(z, 1.0 / 23)
    for p in range(21, 0, -2):
        series = series * z2 + 1.0 / p
    theta = 4.0 * z * series
    gain = 0.5 / jnp.sqrt(alpha * (1.0 + 0.25 * alpha))

    q_one = jnp.exp(-theta)
    place = lax.broadcasted_iota(jnp.int32, (width, extent), 0)
    fplace = place.astype(f32)
    for t in range(rows):
        lanes = slice(t * extent, (t + 1) * extent)
        from_left[:, lanes] = gain[:, lanes] * jnp.exp(-theta[:, lanes] * (fplace + 1.0))
        from_right[:, lanes] = gain[:, lanes] * jnp.exp(-theta[:, lanes] * (width - fplace))
    chunk = jnp.exp(-theta * float(width))
    group = jnp.exp(-theta * float(width * rows))
    whole = jnp.exp(-theta * float(total_cols))

    for copy in first:
        copy.wait_recv()

    length = rows * extent
    partial = jnp.zeros((1, extent), f32)
    for t in range(rows):
        lanes = slice(t * extent, (t + 1) * extent)
        pieces = [in1[d] for d in range(rows)]
        real = weighted_sum(mix_cos[t], pieces)
        imag = weighted_sum(mix_sin[t], pieces)
        high, low = split(jnp.concatenate([real, imag], axis=1))
        both = jnp.dot(
            jnp.concatenate([high, low], axis=0), table_hi[t], preferred_element_type=f32
        )
        value = (
            both[:width] + both[width:] + jnp.dot(high, table_lo[t], preferred_element_type=f32)
        )
        ahead = value
        behind = value
        q = q_one[:, lanes]
        s = 1
        while s < width:
            ahead = ahead + q * jnp.where(place >= s, pltpu.roll(ahead, s, 0), 0.0)
            behind = behind + q * jnp.where(
                place < width - s, pltpu.roll(behind, width - s, 0), 0.0
            )
            q = q * q
            s *= 2
        solved = gain[:, lanes] * (ahead + behind - value)
        partial = partial + jnp.sum(value * solved, axis=0, keepdims=True)
        field[:, lanes] = solved
        rowsum[me_r, 0:1, lanes] = ahead[width - 1 : width]
        rowsum[me_r, 1:2, lanes] = behind[0:1]

    def fold(row):
        return sum(row[:, i : i + 128] for i in range(0, row.shape[1], 128))

    spare = slice(length, length + 128)
    rowsum[me_r, 0:1, spare] = fold(partial)
    rowsum[me_r, 1:2, spare] = jnp.zeros((1, 128), f32)
    mine = rowsum.at[me_r]
    second = share("row", me_r, rows, lambda to: mine, rowsum, s2, r2)

    turn = (((1,), (1,)), ((), ()))
    reals, imags = [], []
    for t in range(rows):
        lanes = slice(t * extent, (t + 1) * extent)
        high, low = split(field[:, lanes])
        both = lax.dot_general(
            jnp.concatenate([high, low], axis=0), table_hi[t], turn, preferred_element_type=f32
        )
        value = (
            both[:width]
            + both[width:]
            + lax.dot_general(high, table_lo[t], turn, preferred_element_type=f32)
        )
        reals.append(value[:, :extent])
        imags.append(value[:, extent:])
    for d in range(rows):
        out2[d] = weighted_sum(list(mix_cos[:, d]) + list(mix_sin[:, d]), reals + imags)
    fifth = share("row", me_r, rows, lambda to: out2.at[to], in2, s5, r5)
    in2[me_r] = out2[me_r]
    for copy in second:
        copy.wait_recv()

    def carries(sums, count, ratio):
        left, right = [jnp.zeros_like(ratio)], [jnp.zeros_like(ratio)]
        for k in range(count):
            left.append(ratio * left[-1] + sums[k, 0:1, :length])
            right.append(ratio * right[-1] + sums[count - 1 - k, 1:2, :length])
        return left[:-1], right[count - 1 :: -1], left[-1], right[-1]

    weight = gain * q_one
    lefts, rights, at_end, at_start = carries(rowsum, rows, chunk)
    coupled = jnp.zeros_like(weight)
    inner = jnp.zeros((1, 128), f32)
    for k in range(rows):
        carry[k, 0:1, :] = lefts[k]
        carry[k, 1:2, :] = rights[k]
        coupled = coupled + lefts[k] * rowsum[k, 1:2, :length] + rights[k] * rowsum[k, 0:1, :length]
        inner = inner + rowsum[k, 0:1, spare]
    colsum[me_c, 0:1, :length] = at_end
    colsum[me_c, 1:2, :length] = at_start
    colsum[me_c, 0:1, spare] = inner + fold(weight * coupled)
    colsum[me_c, 1:2, spare] = jnp.zeros((1, 128), f32)
    mine_c = colsum.at[me_c]
    third = share("col", me_c, cols, lambda to: mine_c, colsum, s3, r3)

    for t in range(rows):
        quads = quadrants(t)
        cos_d, sin_d = f32(mix_cos[t, 0]), f32(mix_sin[t, 0])
        for d in range(1, rows):
            cos_d = jnp.where(me_r == d, f32(mix_cos[t, d]), cos_d)
            sin_d = jnp.where(me_r == d, f32(mix_sin[t, d]), sin_d)
        for j in range(2):
            high, low = split(cos_d * quads[0][j] + sin_d * quads[1][j])
            lanes = slice(t * extent + j * half, t * extent + (j + 1) * half)
            own_hi[:, lanes] = high
            own_lo[:, lanes] = low
    for copy in third:
        copy.wait_recv()

    lefts, rights, at_end, at_start = carries(colsum, cols, group)
    images = 1.0 / (1.0 - whole * whole)
    entry = (at_start + whole * at_end) * images
    exit_ = (at_end + whole * at_start) * images
    for k in range(cols):
        lefts[k] = lefts[k] + entry
        rights[cols - 1 - k] = rights[cols - 1 - k] + exit_
        entry, exit_ = entry * group, exit_ * group
    coupled = jnp.zeros_like(weight)
    inner = jnp.zeros((1, 128), f32)
    left_c, right_c = lefts[0], rights[0]
    for k in range(cols):
        left_c = jnp.where(me_c == k, lefts[k], left_c)
        right_c = jnp.where(me_c == k, rights[k], right_c)
        coupled = coupled + lefts[k] * colsum[k, 1:2, :length] + rights[k] * colsum[k, 0:1, :length]
        inner = inner + colsum[k, 0:1, spare]
    inner = jnp.sum(inner + fold(weight * coupled), axis=1, keepdims=True)
    ratio = inner / scalars_ref[1:2, 0:1]
    ratio_ref[...] = jnp.broadcast_to(ratio, ratio_ref.shape)
    for k in range(rows):
        carry[k, 0:1, :] = carry[k, 0:1, :] + left_c
        carry[rows - 1 - k, 1:2, :] = carry[rows - 1 - k, 1:2, :] + right_c
        left_c, right_c = left_c * chunk, right_c * chunk

    per = 128 // width
    block = out_ref.shape[1]
    for e in range(0, out_ref.shape[1], block):
        for r in range(e // width, (e + block) // width):
            at = slice(r * width, (r + 1) * width)
            for t in range(rows):
                lanes = slice(t * extent, (t + 1) * extent)
                high, low = split(
                    from_left[:, lanes] * carry[r, 0:1, lanes]
                    + from_right[:, lanes] * carry[r, 1:2, lanes]
                )
                carried_hi[at, lanes] = high
                carried_lo[at, lanes] = low
        at = slice(e, e + block)
        added[at, :] = (
            lax.dot_general(carried_hi[at, :], own_hi[...], turn, preferred_element_type=f32)
            + lax.dot_general(carried_lo[at, :], own_hi[...], turn, preferred_element_type=f32)
            + lax.dot_general(carried_hi[at, :], own_lo[...], turn, preferred_element_type=f32)
        )
    for copy in fifth:
        copy.wait_recv()
    for e in range(0, out_ref.shape[1], 128):
        turned = jnp.concatenate([in2[e // width + i] for i in range(per)], axis=0)
        turned = turned + added[e : e + 128, :]
        out_ref[:, e : e + 128] = turned.T
    for copies in (first, second, third, fifth):
        for copy in copies:
            copy.wait_send()


def body(rows, cols, residual, direction, ground_shift, previous):
    extent, here = residual.shape
    width = here // rows
    length = extent * rows
    f32 = jnp.float32
    coarse, fine, eigen = base_tables(extent, rows)
    vmem = pl.BlockSpec(memory_space=pltpu.VMEM)
    smem = pl.BlockSpec(memory_space=pltpu.SMEM)
    dma = pltpu.SemaphoreType.DMA
    per_row, per_col = max(rows - 1, 1), max(cols - 1, 1)
    hbm = pl.BlockSpec(memory_space=pltpu.HBM)
    scratch = [
        pltpu.VMEM((extent, here), f32),
        pltpu.VMEM(coarse.shape, f32),
        pltpu.VMEM(fine.shape, f32),
        pltpu.VMEM(eigen.shape, f32),
        dma((4,)),
        pltpu.VMEM((rows, width, extent), f32),
        pltpu.VMEM((rows, width, extent), f32),
        pltpu.VMEM((rows, width, extent), f32),
        pltpu.VMEM((rows, width, extent), f32),
        pltpu.VMEM((rows, 2 * extent, extent), jnp.bfloat16),
        pltpu.VMEM((rows, 2 * extent, extent), jnp.bfloat16),
        pltpu.VMEM((width, length), f32),
        pltpu.VMEM((width, length), f32),
        pltpu.VMEM((width, length), f32),
        pltpu.VMEM((extent, length), jnp.bfloat16),
        pltpu.VMEM((extent, length), jnp.bfloat16),
        pltpu.VMEM((here, length), jnp.bfloat16),
        pltpu.VMEM((here, length), jnp.bfloat16),
        pltpu.VMEM((here, extent), f32),
        pltpu.VMEM((rows, 2, length + 128), f32),
        pltpu.VMEM((cols, 2, length + 128), f32),
        pltpu.VMEM((rows, 2, length), f32),
        dma((per_row,)),
        dma((per_row,)),
        dma((per_row,)),
        dma((per_row,)),
        dma((per_col,)),
        dma((per_col,)),
        dma((per_row,)),
        dma((per_row,)),
    ]
    held = sum(
        math.prod(ref.shape) * jnp.dtype(ref.dtype).itemsize
        for ref in scratch
        if ref.memory_space == pltpu.VMEM
    )
    scalars = jnp.broadcast_to(jnp.stack([ground_shift, previous]), (2, 128))
    operands = (residual, coarse, fine, eigen)
    solved, ratio = pl.pallas_call(
        functools.partial(kernel, rows, cols),
        out_shape=(
            jax.ShapeDtypeStruct((extent, here), f32),
            jax.ShapeDtypeStruct((1, 128), f32),
        ),
        in_specs=[hbm] * 4 + [vmem],
        out_specs=(vmem, vmem),
        scratch_shapes=scratch,
        compiler_params=pltpu.CompilerParams(
            collective_id=0,
            has_side_effects=True,
            vmem_limit_bytes=min(held + (held >> 2) + (4 << 20), 60 << 20),
        ),
    )(*(pltpu.with_memory_space_constraint(x, pltpu.HBM) for x in operands), scalars)
    return pl.pallas_call(
        update,
        out_shape=(
            jax.ShapeDtypeStruct((extent, here), f32),
            jax.ShapeDtypeStruct((1,), f32),
        ),
        in_specs=[vmem, vmem, vmem],
        out_specs=(vmem, smem),
        compiler_params=pltpu.CompilerParams(vmem_limit_bytes=8 * 1024 * 1024),
    )(solved, direction, ratio)


def update(solved_ref, direction_ref, ratio_in, out_ref, ratio_out):
    ratio = ratio_in[0:1, 0:1]
    out_ref[...] = solved_ref[...] + ratio * direction_ref[...]
    ratio_out[0] = ratio_in[0, 0]


def solution(mesh):
    return jax.shard_map(
        functools.partial(body, mesh.shape["row"], mesh.shape["col"]),
        mesh=mesh,
        in_specs=(P("row", "col"), P("row", "col"), P(), P()),
        out_specs=(P("row", "col"), P()),
        check_vma=False,
    )
```

```python
import functools
import math

import jax
import jax.numpy as jnp
import numpy as np
from jax import lax
from jax.experimental import pallas as pl
from jax.experimental.pallas import tpu as pltpu
from jax.sharding import PartitionSpec as P

MESH = pl.DeviceIdType.MESH
HALVES = 2


def halves_of(table):
    high = table.astype(jnp.bfloat16)
    low = (table - high.astype(np.float64)).astype(jnp.bfloat16)
    return np.stack([high, low])


def sine_table(extent):
    index = np.arange(1, extent + 1, dtype=np.int64)
    turns = index[:, None] * index[None, :] % (2 * (extent + 1))
    table = math.sqrt(2.0 / (extent + 1)) * np.sin(np.pi * turns / (extent + 1))
    eigen = 4.0 * np.sin(np.pi * index / (2 * (extent + 1))) ** 2
    return halves_of(table), eigen


def tables(extent, width, cols):
    length = width * cols
    modes = np.arange(length, dtype=np.int64)[None, :]
    coarse = 64 * np.arange(length // 64, dtype=np.int64)[:, None]
    middle = 8 * np.arange(8, dtype=np.int64)[:, None]
    fine = 2 * np.arange(8, dtype=np.int64)[:, None] + 1
    coarse = np.pi * (modes * coarse % (2 * length)) / length
    middle = np.pi * (modes * middle % (2 * length)) / length
    fine = np.pi * (modes * fine % (4 * length)) / (2 * length)
    scale = np.where(modes == 0, math.sqrt(1.0 / length), math.sqrt(2.0 / length))
    far = np.stack([np.cos(coarse), np.sin(coarse)]).astype(np.float32)
    near = np.stack(
        [np.cos(middle), np.sin(middle), scale * np.cos(fine), scale * np.sin(fine)]
    ).astype(np.float32)
    waves = 4.0 * np.sin(np.pi * modes / (2 * length)) ** 2
    row_sines, row_eigen = sine_table(extent)
    col_sines, col_eigen = sine_table(width)
    both = (col_eigen[:, None] + row_eigen[None, :]).astype(np.float32)
    return (
        far,
        near,
        waves.reshape(-1, 128).astype(np.float32),
        row_eigen[None, :].astype(np.float32),
        both,
        row_sines,
        col_sines,
    )


def split(value):
    high = value.astype(jnp.bfloat16)
    return high, (value - high.astype(jnp.float32)).astype(jnp.bfloat16)


def decay(alpha):
    h = 0.5 * jnp.sqrt(alpha)
    z = h / (1.0 + jnp.sqrt(1.0 + h * h))
    z2 = z * z
    series = jnp.full_like(z, 1.0 / 23)
    for p in range(21, 0, -2):
        series = series * z2 + 1.0 / p
    return 4.0 * z * series, 0.5 / jnp.sqrt(alpha * (1.0 + 0.25 * alpha))


def waves(ps, qs, chunk, whole):
    count = len(ps)
    fronts, backs = [], [None] * count
    left, right = jnp.zeros_like(chunk), jnp.zeros_like(chunk)
    for k in range(count):
        fronts.append(left)
        left = chunk * left + qs[k]
        backs[count - 1 - k] = right
        right = chunk * right + ps[count - 1 - k]
    images = 1.0 / (1.0 - whole * whole)
    entry = (right + whole * left) * images
    exit_ = (left + whole * right) * images
    for k in range(count):
        fronts[k] = fronts[k] + entry
        backs[count - 1 - k] = backs[count - 1 - k] + exit_
        entry, exit_ = entry * chunk, exit_ * chunk
    return fronts, backs


def amplitudes(ps, qs, theta, gain, extent, me):
    count = len(ps)
    fronts, backs = waves(
        ps, qs, jnp.exp(-theta * float(extent)), jnp.exp(-theta * float(extent * count))
    )
    far = jnp.exp(-theta * float(extent + 1))
    inside = gain / (1.0 - far * far)
    outside = gain * jnp.exp(theta)
    total = jnp.zeros_like(theta)
    mine_a, mine_b = jnp.zeros_like(theta), jnp.zeros_like(theta)
    for k in range(count):
        a = outside * fronts[k] + inside * (ps[k] - far * qs[k])
        b = outside * backs[k] + inside * (qs[k] - far * ps[k])
        total = total + a * ps[k] + b * qs[k]
        mine_a = jnp.where(me == k, a, mine_a)
        mine_b = jnp.where(me == k, b, mine_b)
    return mine_a, mine_b, total


def fill_decays(theta_rows, down_ref, up_ref):
    blocks = down_ref.shape[0] // 8
    tiles = len(theta_rows)
    place = lax.broadcasted_iota(jnp.int32, (8, 128), 0).astype(jnp.float32)
    for first in range(0, tiles, 8):
        group = range(first, min(first + 8, tiles))
        steps = [jnp.exp(-8.0 * jnp.broadcast_to(theta_rows[t], (8, 128))) for t in group]
        down = [jnp.exp(-theta_rows[t] * (place + 1.0)) for t in group]
        up = [jnp.exp(-theta_rows[t] * (8.0 - place)) for t in group]

        def step(n, carry):
            down, up = carry
            top = pl.ds(pl.multiple_of(8 * n, 8), 8)
            bottom = pl.ds(pl.multiple_of(8 * (blocks - 1 - n), 8), 8)
            for i, t in enumerate(group):
                down_ref[top, t * 128 : (t + 1) * 128] = down[i]
                up_ref[bottom, t * 128 : (t + 1) * 128] = up[i]
            return (
                [d * s for d, s in zip(down, steps)],
                [u * s for u, s in zip(up, steps)],
            )

        lax.fori_loop(0, blocks, step, (down, up))


def kernel(
    rows,
    cols,
    residual_hbm,
    far_hbm,
    near_hbm,
    waves_hbm,
    row_eigen_hbm,
    both_hbm,
    row_sines_hbm,
    col_sines_hbm,
    scalars_ref,
    out_ref,
    ratio_ref,
    residual_ref,
    far_ref,
    near_ref,
    waves_ref,
    row_eigen_ref,
    both_ref,
    row_sines_ref,
    col_sines_ref,
    load_sems,
    theta_ref,
    cos_ref,
    sin_ref,
    table_hi,
    table_lo,
    down,
    up,
    side_down,
    side_up,
    amp_ref,
    col_in,
    carry_in,
    row_in,
    quad_in,
    s_col,
    r_col,
    s_carry,
    r_carry,
    s_row,
    r_row,
    s_quad,
    r_quad,
):
    me_r = lax.axis_index("row")
    me_c = lax.axis_index("col")
    extent, width = residual_ref.shape
    length = table_hi.shape[1]
    tiles = length // 128
    part = tiles // HALVES
    f32 = jnp.float32

    barrier = pltpu.get_barrier_semaphore()
    for o in range(1, cols):
        pl.semaphore_signal(
            barrier, inc=1, device_id={"col": lax.rem(me_c + o, cols)}, device_id_type=MESH
        )
    for o in range(1, rows):
        pl.semaphore_signal(
            barrier, inc=1, device_id={"row": lax.rem(me_r + o, rows)}, device_id_type=MESH
        )

    per = width // 64
    own = far_hbm.at[:, pl.ds(pl.multiple_of(me_c * per, per), per), :]
    loads = []
    for i, (source, landing) in enumerate(
        (
            (waves_hbm, waves_ref),
            (near_hbm, near_ref),
            (own, far_ref),
            (residual_hbm, residual_ref),
            (row_eigen_hbm, row_eigen_ref),
            (row_sines_hbm, row_sines_ref),
            (col_sines_hbm, col_sines_ref),
            (both_hbm, both_ref),
        )
    ):
        copy = pltpu.make_async_copy(source, landing, load_sems.at[i])
        copy.start()
        loads.append(copy)

    def share(axis, me, count, ref, send_sems, recv_sems, first=0):
        copies = []
        for o in range(1, count):
            copy = pltpu.make_async_remote_copy(
                src_ref=ref,
                dst_ref=ref,
                send_sem=send_sems.at[first + o - 1],
                recv_sem=recv_sems.at[first + o - 1],
                device_id={axis: lax.rem(me + o, count)},
                device_id_type=MESH,
            )
            copy.start()
            copies.append(copy)
        return copies

    shift = scalars_ref[0:1, 0:1]
    loads[0].wait()
    theta, gain = decay(waves_ref[...] + shift)
    theta_ref[...] = theta
    fill_decays([theta_ref[t : t + 1, :] for t in range(tiles)], down, up)

    loads[1].wait()
    loads[2].wait()
    for u in range(per):
        rows_u = slice(8 * u, 8 * u + 8)
        cos_u, sin_u = far_ref[0, u : u + 1, :], far_ref[1, u : u + 1, :]
        cos_ref[rows_u, :] = cos_u * near_ref[0] - sin_u * near_ref[1]
        sin_ref[rows_u, :] = sin_u * near_ref[0] + cos_u * near_ref[1]

    span = min(1024, length)

    def fill(n, carry):
        at = pl.ds(pl.multiple_of(16 * n, 16), 16)
        for first in range(0, length, span):
            lanes = slice(first, first + span)
            pieces = []
            for k in range(2):
                row = pl.ds(2 * n + k, 1)
                pieces.append(
                    cos_ref[row, lanes] * near_ref[2, :, lanes]
                    - sin_ref[row, lanes] * near_ref[3, :, lanes]
                )
            high, low = split(jnp.concatenate(pieces, axis=0))
            table_hi[at, lanes] = high
            table_lo[at, lanes] = low
        return carry

    lax.fori_loop(0, width // 16, fill, 0)

    loads[3].wait()
    r_hi, r_lo = split(residual_ref[...])
    stacked = jnp.concatenate([r_hi, r_lo, r_hi], axis=1)
    for first in range(0, length, 256):
        lanes = slice(first, first + 256)
        high, low = table_hi[:, lanes], table_lo[:, lanes]
        value = jnp.dot(
            stacked, jnp.concatenate([high, high, low], axis=0), preferred_element_type=f32
        )
        p = jnp.sum(value * down[:, lanes], axis=0, keepdims=True)
        q = jnp.sum(value * up[:, lanes], axis=0, keepdims=True)
        for i in range(2):
            half, at = divmod(first // 128 + i, part)
            piece = slice(128 * i, 128 * i + 128)
            col_in[me_c, half, at : at + 1, :] = p[:, piece]
            col_in[me_c, half, part + at : part + at + 1, :] = q[:, piece]

    pl.semaphore_wait(barrier, rows + cols - 2)
    col_copies = [
        share("col", me_c, cols, col_in.at[me_c, h], s_col, r_col, h * (cols - 1))
        for h in range(HALVES)
    ]

    for copy in loads[4:]:
        copy.wait()
    left = (((0,), (0,)), ((), ()))
    turn = (((1,), (1,)), ((), ()))
    modal = lax.dot_general(
        jnp.concatenate([r_hi, r_lo, r_hi], axis=0),
        jnp.concatenate([row_sines_ref[0], row_sines_ref[0], row_sines_ref[1]], axis=0),
        left,
        preferred_element_type=f32,
    )
    phi, side_gain = decay(row_eigen_ref[...] + shift)
    fill_decays(
        [phi[:, e : e + 128] for e in range(0, extent, 128)], side_down, side_up
    )
    carry_in[me_c, 0:1, :] = jnp.sum(modal * side_down[...], axis=0, keepdims=True)
    carry_in[me_c, 1:2, :] = jnp.sum(modal * side_up[...], axis=0, keepdims=True)
    sines = jnp.concatenate([col_sines_ref[0], col_sines_ref[0], col_sines_ref[1]], axis=1)

    def across(value):
        high, low = split(value)
        return jnp.dot(
            sines, jnp.concatenate([high, low, high], axis=0), preferred_element_type=f32
        )

    spectrum = across(modal)
    scaled = spectrum / (both_ref[...] + shift)
    carry_in[me_c, 2:3, :] = jnp.sum(spectrum * scaled, axis=0, keepdims=True)
    carry_in[me_c, 3:4, :] = jnp.zeros((1, extent), f32)
    carry_copies = share("col", me_c, cols, carry_in.at[me_c], s_carry, r_carry)
    field = across(scaled)

    row_copies = []
    for h in range(HALVES):
        for copy in col_copies[h]:
            copy.wait_recv()
        total = col_in[0, h]
        for k in range(1, cols):
            total = total + col_in[k, h]
        row_in[me_r, h] = total
        row_copies.append(
            share("row", me_r, rows, row_in.at[me_r, h], s_row, r_row, h * (rows - 1))
        )

    for copy in carry_copies:
        copy.wait_recv()
    a, b, quad = amplitudes(
        [carry_in[k, 0:1, :] for k in range(cols)],
        [carry_in[k, 1:2, :] for k in range(cols)],
        phi,
        side_gain,
        width,
        me_c,
    )
    for k in range(cols):
        quad = quad + carry_in[k, 2:3, :]
    quad_in[me_r] = sum(quad[:, e : e + 128] for e in range(0, extent, 128))
    quad_copies = share("row", me_r, rows, quad_in.at[me_r], s_quad, r_quad)
    high, low = split(field + a * side_down[...] + b * side_up[...])
    out_ref[...] = lax.dot_general(
        jnp.concatenate([row_sines_ref[0], row_sines_ref[0], row_sines_ref[1]], axis=1),
        jnp.concatenate([high, low, high], axis=1),
        turn,
        preferred_element_type=f32,
    )

    inner = jnp.zeros((part, 128), f32)
    for h in range(HALVES):
        for copy in row_copies[h]:
            copy.wait_recv()
        at = slice(h * part, (h + 1) * part)
        a, b, quad = amplitudes(
            [row_in[k, h, :part] for k in range(rows)],
            [row_in[k, h, part:] for k in range(rows)],
            theta[at],
            gain[at],
            extent,
            me_r,
        )
        inner = inner + quad
        amp_ref[0, at] = a
        amp_ref[1, at] = b
        for first in range(h * part * 128, (h + 1) * part * 128, 256):
            lanes = slice(first, first + 256)
            t = first // 128
            a_row = jnp.concatenate([amp_ref[0, t + i : t + i + 1, :] for i in range(2)], axis=1)
            b_row = jnp.concatenate([amp_ref[1, t + i : t + i + 1, :] for i in range(2)], axis=1)
            high, low = split(a_row * down[:, lanes] + b_row * up[:, lanes])
            t_hi, t_lo = table_hi[:, lanes], table_lo[:, lanes]
            out_ref[...] += lax.dot_general(
                jnp.concatenate([high, low, high], axis=1),
                jnp.concatenate([t_hi, t_hi, t_lo], axis=1),
                turn,
                preferred_element_type=f32,
            )

    for copy in quad_copies:
        copy.wait_recv()
    inner = jnp.sum(inner, axis=0, keepdims=True)
    for k in range(rows):
        inner = inner + quad_in[k]
    ratio = jnp.sum(inner, axis=1, keepdims=True) / scalars_ref[1:2, 0:1]
    ratio_ref[...] = jnp.broadcast_to(ratio, ratio_ref.shape)
    for copies in (*col_copies, carry_copies, *row_copies, quad_copies):
        for copy in copies:
            copy.wait_send()


def body(rows, cols, residual, direction, ground_shift, previous):
    extent, width = residual.shape
    length = width * cols
    f32, bf16 = jnp.float32, jnp.bfloat16
    constants = tables(extent, width, cols)
    vmem = pl.BlockSpec(memory_space=pltpu.VMEM)
    smem = pl.BlockSpec(memory_space=pltpu.SMEM)
    hbm = pl.BlockSpec(memory_space=pltpu.HBM)
    dma = pltpu.SemaphoreType.DMA
    per_row, per_col = max(rows - 1, 1), max(cols - 1, 1)
    operands = (residual, *constants)
    scalars = jnp.broadcast_to(jnp.stack([ground_shift, previous]), (2, 128))
    tiles = length // 128
    part = tiles // HALVES
    landings = [
        pltpu.VMEM((2, width // 64, length) if i == 1 else x.shape, x.dtype)
        for i, x in enumerate(operands)
    ]
    scratch = landings + [
        dma((len(operands),)),
        pltpu.VMEM((tiles, 128), f32),
        pltpu.VMEM((width // 8, length), f32),
        pltpu.VMEM((width // 8, length), f32),
        pltpu.VMEM((width, length), bf16),
        pltpu.VMEM((width, length), bf16),
        pltpu.VMEM((extent, length), f32),
        pltpu.VMEM((extent, length), f32),
        pltpu.VMEM((width, extent), f32),
        pltpu.VMEM((width, extent), f32),
        pltpu.VMEM((2, tiles, 128), f32),
        pltpu.VMEM((cols, HALVES, 2 * part, 128), f32),
        pltpu.VMEM((cols, 4, extent), f32),
        pltpu.VMEM((rows, HALVES, 2 * part, 128), f32),
        pltpu.VMEM((rows, 1, 128), f32),
        dma((HALVES * per_col,)),
        dma((HALVES * per_col,)),
        dma((per_col,)),
        dma((per_col,)),
        dma((HALVES * per_row,)),
        dma((HALVES * per_row,)),
        dma((per_row,)),
        dma((per_row,)),
    ]
    held = sum(
        math.prod(ref.shape) * jnp.dtype(ref.dtype).itemsize
        for ref in scratch
        if ref.memory_space == pltpu.VMEM
    )
    solved, ratio = pl.pallas_call(
        functools.partial(kernel, rows, cols),
        out_shape=(
            jax.ShapeDtypeStruct((extent, width), f32),
            jax.ShapeDtypeStruct((1, 128), f32),
        ),
        in_specs=[hbm] * len(operands) + [vmem],
        out_specs=(vmem, vmem),
        scratch_shapes=scratch,
        compiler_params=pltpu.CompilerParams(
            collective_id=0,
            has_side_effects=True,
            vmem_limit_bytes=min(held + (held >> 2) + (8 << 20), 61 << 20),
        ),
    )(*(pltpu.with_memory_space_constraint(x, pltpu.HBM) for x in operands), scalars)
    return pl.pallas_call(
        update,
        out_shape=(
            jax.ShapeDtypeStruct((extent, width), f32),
            jax.ShapeDtypeStruct((1,), f32),
        ),
        in_specs=[vmem, vmem, vmem],
        out_specs=(vmem, smem),
        compiler_params=pltpu.CompilerParams(vmem_limit_bytes=8 << 20),
    )(solved, direction, ratio)


def update(solved_ref, direction_ref, ratio_in, out_ref, ratio_out):
    ratio = ratio_in[0:1, 0:1]
    out_ref[...] = solved_ref[...] + ratio * direction_ref[...]
    ratio_out[0] = ratio_in[0, 0]


def solution(mesh):
    return jax.shard_map(
        functools.partial(body, mesh.shape["row"], mesh.shape["col"]),
        mesh=mesh,
        in_specs=(P("row", "col"), P("row", "col"), P(), P()),
        out_specs=(P("row", "col"), P()),
        check_vma=False,
    )
```

```python
import functools
import math

import jax
import jax.numpy as jnp
import numpy as np
from jax import lax
from jax.experimental import pallas as pl
from jax.experimental.pallas import tpu as pltpu
from jax.sharding import PartitionSpec as P

MESH = pl.DeviceIdType.MESH
HALVES = 2


def halves_of(table):
    high = table.astype(jnp.bfloat16)
    low = (table - high.astype(np.float64)).astype(jnp.bfloat16)
    return np.stack([high, low])


def sine_table(extent):
    index = np.arange(1, extent + 1, dtype=np.int64)
    turns = index[:, None] * index[None, :] % (2 * (extent + 1))
    table = math.sqrt(2.0 / (extent + 1)) * np.sin(np.pi * turns / (extent + 1))
    eigen = 4.0 * np.sin(np.pi * index / (2 * (extent + 1))) ** 2
    return halves_of(table), eigen


def column_cosines(width, cols):
    length = width * cols
    modes = np.arange(length, dtype=np.int64)[None, :]
    odd = 2 * np.arange(length, dtype=np.int64)[:, None] + 1
    scale = np.where(modes == 0, math.sqrt(1.0 / length), math.sqrt(2.0 / length))
    table = scale * np.cos(np.pi * (modes * odd % (4 * length)) / (2 * length))
    return halves_of(table).reshape(2, cols, width, length).swapaxes(0, 1)


def tables(extent, width, cols, ready):
    length = width * cols
    modes = np.arange(length, dtype=np.int64)[None, :]
    coarse = 64 * np.arange(length // 64, dtype=np.int64)[:, None]
    middle = 8 * np.arange(8, dtype=np.int64)[:, None]
    fine = 2 * np.arange(8, dtype=np.int64)[:, None] + 1
    coarse = np.pi * (modes * coarse % (2 * length)) / length
    middle = np.pi * (modes * middle % (2 * length)) / length
    fine = np.pi * (modes * fine % (4 * length)) / (2 * length)
    scale = np.where(modes == 0, math.sqrt(1.0 / length), math.sqrt(2.0 / length))
    far = np.stack([np.cos(coarse), np.sin(coarse)]).astype(np.float32)
    near = np.stack(
        [np.cos(middle), np.sin(middle), scale * np.cos(fine), scale * np.sin(fine)]
    ).astype(np.float32)
    waves = 4.0 * np.sin(np.pi * modes / (2 * length)) ** 2
    row_sines, row_eigen = sine_table(extent)
    col_sines, col_eigen = sine_table(width)
    both = (col_eigen[:, None] + row_eigen[None, :]).astype(np.float32)
    sources = (column_cosines(width, cols),) if ready else (far, near)
    return (
        waves.reshape(-1, 128).astype(np.float32),
        row_eigen[None, :].astype(np.float32),
        both,
        row_sines,
        col_sines,
        *sources,
    )


def split(value):
    high = value.astype(jnp.bfloat16)
    return high, (value - high.astype(jnp.float32)).astype(jnp.bfloat16)


def decay(alpha):
    h = 0.5 * jnp.sqrt(alpha)
    z = h / (1.0 + jnp.sqrt(1.0 + h * h))
    z2 = z * z
    series = jnp.full_like(z, 1.0 / 23)
    for p in range(21, 0, -2):
        series = series * z2 + 1.0 / p
    return 4.0 * z * series, 0.5 / jnp.sqrt(alpha * (1.0 + 0.25 * alpha))


def waves(ps, qs, chunk, whole):
    count = len(ps)
    fronts, backs = [], [None] * count
    left, right = jnp.zeros_like(chunk), jnp.zeros_like(chunk)
    for k in range(count):
        fronts.append(left)
        left = chunk * left + qs[k]
        backs[count - 1 - k] = right
        right = chunk * right + ps[count - 1 - k]
    images = 1.0 / (1.0 - whole * whole)
    entry = (right + whole * left) * images
    exit_ = (left + whole * right) * images
    for k in range(count):
        fronts[k] = fronts[k] + entry
        backs[count - 1 - k] = backs[count - 1 - k] + exit_
        entry, exit_ = entry * chunk, exit_ * chunk
    return fronts, backs


def amplitudes(ps, qs, theta, gain, extent, me):
    count = len(ps)
    fronts, backs = waves(
        ps, qs, jnp.exp(-theta * float(extent)), jnp.exp(-theta * float(extent * count))
    )
    far = jnp.exp(-theta * float(extent + 1))
    inside = gain / (1.0 - far * far)
    outside = gain * jnp.exp(theta)
    total = jnp.zeros_like(theta)
    mine_a, mine_b = jnp.zeros_like(theta), jnp.zeros_like(theta)
    for k in range(count):
        a = outside * fronts[k] + inside * (ps[k] - far * qs[k])
        b = outside * backs[k] + inside * (qs[k] - far * ps[k])
        total = total + a * ps[k] + b * qs[k]
        mine_a = jnp.where(me == k, a, mine_a)
        mine_b = jnp.where(me == k, b, mine_b)
    return mine_a, mine_b, total


def fill_decays(theta_rows, down_ref, up_ref):
    blocks = down_ref.shape[0] // 8
    tiles = len(theta_rows)
    place = lax.broadcasted_iota(jnp.int32, (8, 128), 0).astype(jnp.float32)
    for first in range(0, tiles, 8):
        group = range(first, min(first + 8, tiles))
        steps = [jnp.exp(-8.0 * jnp.broadcast_to(theta_rows[t], (8, 128))) for t in group]
        down = [jnp.exp(-theta_rows[t] * (place + 1.0)) for t in group]
        up = [jnp.exp(-theta_rows[t] * (8.0 - place)) for t in group]

        def step(n, carry):
            down, up = carry
            top = pl.ds(pl.multiple_of(8 * n, 8), 8)
            bottom = pl.ds(pl.multiple_of(8 * (blocks - 1 - n), 8), 8)
            for i, t in enumerate(group):
                down_ref[top, t * 128 : (t + 1) * 128] = down[i]
                up_ref[bottom, t * 128 : (t + 1) * 128] = up[i]
            return (
                [d * s for d, s in zip(down, steps)],
                [u * s for u, s in zip(up, steps)],
            )

        lax.fori_loop(0, blocks, step, (down, up))


def kernel(rows, cols, ready, *refs):
    def run(*sums):
        apply(rows, cols, ready, sums, *refs)

    extent = refs[0].shape[0]
    pl.run_scoped(run, *(pltpu.ACC(m)((extent, 256), jnp.float32) for m in (0, 0, 1, 1)))


def multiply(total, unit, right, left, transpose=False):
    high, low = left
    pltpu.matmul_push_rhs(right[0], 0, unit, transpose=transpose)
    pltpu.matmul_acc_lhs(total, high, load_staged_rhs=0)
    pltpu.matmul_acc_lhs(total, low)
    pltpu.matmul_push_rhs(right[1], 1, unit, transpose=transpose)
    pltpu.matmul_acc_lhs(total, high, load_staged_rhs=1)


def apply(rows, cols, ready, sums, *refs):
    sources = 1 if ready else 2
    residual_hbm, waves_hbm, row_eigen_hbm, both_hbm, row_sines_hbm, col_sines_hbm = refs[:6]
    source_hbms = refs[6 : 6 + sources]
    scalars_ref, out_ref, ratio_ref = refs[6 + sources : 9 + sources]
    residual_ref, waves_ref, row_eigen_ref, both_ref, row_sines_ref, col_sines_ref = refs[
        9 + sources : 15 + sources
    ]
    (
        load_sems,
        theta_ref,
        table,
        down,
        up,
        side_down,
        side_up,
        amp_ref,
        col_in,
        carry_in,
        row_in,
        quad_in,
        s_col,
        r_col,
        s_carry,
        r_carry,
        s_row,
        r_row,
        s_quad,
        r_quad,
        *spare,
    ) = refs[15 + sources :]
    me_r = lax.axis_index("row")
    me_c = lax.axis_index("col")
    extent, width = residual_ref.shape
    length = table.shape[2]
    tiles = length // 128
    part = tiles // HALVES
    f32 = jnp.float32

    barrier = pltpu.get_barrier_semaphore()
    for o in range(1, cols):
        pl.semaphore_signal(
            barrier, inc=1, device_id={"col": lax.rem(me_c + o, cols)}, device_id_type=MESH
        )
    for o in range(1, rows):
        pl.semaphore_signal(
            barrier, inc=1, device_id={"row": lax.rem(me_r + o, rows)}, device_id_type=MESH
        )

    loads = []

    def load(source, landing):
        copy = pltpu.make_async_copy(source, landing, load_sems.at[len(loads)])
        copy.start()
        loads.append(copy)
        return copy

    waves_load = load(waves_hbm, waves_ref)
    residual_load = load(residual_hbm, residual_ref)
    chunk = min(512, length)
    table_loads = []
    if ready:
        for first in range(0, length, chunk):
            lanes = slice(first, first + chunk)
            table_loads.append(load(source_hbms[0].at[me_c, :, :, lanes], table.at[:, :, lanes]))
    else:
        far_ref, near_ref, cos_ref, sin_ref = spare
        per = width // 64
        own = source_hbms[0].at[:, pl.ds(pl.multiple_of(me_c * per, per), per), :]
        far_load = load(own, far_ref)
        near_load = load(source_hbms[1], near_ref)
    late_loads = [
        load(source, landing)
        for source, landing in (
            (row_eigen_hbm, row_eigen_ref),
            (row_sines_hbm, row_sines_ref),
            (col_sines_hbm, col_sines_ref),
            (both_hbm, both_ref),
        )
    ]

    def share(axis, me, count, ref, send_sems, recv_sems, first=0):
        copies = []
        for o in range(1, count):
            copy = pltpu.make_async_remote_copy(
                src_ref=ref,
                dst_ref=ref,
                send_sem=send_sems.at[first + o - 1],
                recv_sem=recv_sems.at[first + o - 1],
                device_id={axis: lax.rem(me + o, count)},
                device_id_type=MESH,
            )
            copy.start()
            copies.append(copy)
        return copies

    shift = scalars_ref[0:1, 0:1]
    waves_load.wait()
    theta, gain = decay(waves_ref[...] + shift)
    theta_ref[...] = theta
    fill_decays([theta_ref[t : t + 1, :] for t in range(tiles)], down, up)

    if not ready:
        far_load.wait()
        near_load.wait()
        for u in range(per):
            rows_u = slice(8 * u, 8 * u + 8)
            cos_u, sin_u = far_ref[0, u : u + 1, :], far_ref[1, u : u + 1, :]
            cos_ref[rows_u, :] = cos_u * near_ref[0] - sin_u * near_ref[1]
            sin_ref[rows_u, :] = sin_u * near_ref[0] + cos_u * near_ref[1]

        span = min(1024, length)

        def fill(n, carry):
            at = pl.ds(pl.multiple_of(16 * n, 16), 16)
            for first in range(0, length, span):
                lanes = slice(first, first + span)
                pieces = []
                for k in range(2):
                    row = pl.ds(2 * n + k, 1)
                    pieces.append(
                        cos_ref[row, lanes] * near_ref[2, :, lanes]
                        - sin_ref[row, lanes] * near_ref[3, :, lanes]
                    )
                high, low = split(jnp.concatenate(pieces, axis=0))
                table[0, at, lanes] = high
                table[1, at, lanes] = low
            return carry

        lax.fori_loop(0, width // 16, fill, 0)

    residual_load.wait()
    r_hi, r_lo = split(residual_ref[...])
    for tile in range(length // 256):
        lanes = slice(256 * tile, 256 * tile + 256)
        if ready and tile in (0, 4):
            for copy in table_loads[: 2] if tile == 0 else table_loads[2:]:
                copy.wait()
        unit = tile % 2
        total = sums[2 * unit + tile // 2 % 2]
        for first in range(0, width, 256):
            at = slice(first, first + 256)
            multiply(
                total,
                unit,
                (table[0, at, lanes], table[1, at, lanes]),
                (r_hi[:, at], r_lo[:, at]),
            )
        value = pltpu.matmul_pop(total)
        p = jnp.sum(value * down[:, lanes], axis=0, keepdims=True)
        q = jnp.sum(value * up[:, lanes], axis=0, keepdims=True)
        for i in range(2):
            half, at = divmod(2 * tile + i, part)
            piece = slice(128 * i, 128 * i + 128)
            col_in[me_c, half, at : at + 1, :] = p[:, piece]
            col_in[me_c, half, part + at : part + at + 1, :] = q[:, piece]

    pl.semaphore_wait(barrier, rows + cols - 2)
    col_copies = [
        share("col", me_c, cols, col_in.at[me_c, h], s_col, r_col, h * (cols - 1))
        for h in range(HALVES)
    ]

    for copy in late_loads:
        copy.wait()
    turned_hi, turned_lo = split(residual_ref[...].T)
    tops = [slice(256 * unit, 256 * unit + 256) for unit in range(2)]
    for unit in range(2):
        multiply(
            sums[2 * unit],
            unit,
            (row_sines_ref[0], row_sines_ref[1]),
            (turned_hi[tops[unit]], turned_lo[tops[unit]]),
        )
    modal = jnp.concatenate([pltpu.matmul_pop(sums[2 * unit]) for unit in range(2)], axis=0)
    phi, side_gain = decay(row_eigen_ref[...] + shift)
    fill_decays(
        [phi[:, e : e + 128] for e in range(0, extent, 128)], side_down, side_up
    )
    carry_in[me_c, 0:1, :] = jnp.sum(modal * side_down[...], axis=0, keepdims=True)
    carry_in[me_c, 1:2, :] = jnp.sum(modal * side_up[...], axis=0, keepdims=True)

    def across(value):
        high, low = split(value)
        for unit in range(2):
            for at in tops:
                multiply(
                    sums[2 * unit],
                    unit,
                    (high[at], low[at]),
                    (col_sines_ref[0, tops[unit], at], col_sines_ref[1, tops[unit], at]),
                )
        return jnp.concatenate([pltpu.matmul_pop(sums[2 * unit]) for unit in range(2)], axis=0)

    spectrum = across(modal)
    scaled = spectrum / (both_ref[...] + shift)
    carry_in[me_c, 2:3, :] = jnp.sum(spectrum * scaled, axis=0, keepdims=True)
    carry_in[me_c, 3:4, :] = jnp.zeros((1, extent), f32)
    carry_copies = share("col", me_c, cols, carry_in.at[me_c], s_carry, r_carry)
    field = across(scaled)

    row_copies = []
    for h in range(HALVES):
        for copy in col_copies[h]:
            copy.wait_recv()
        total = col_in[0, h]
        for k in range(1, cols):
            total = total + col_in[k, h]
        row_in[me_r, h] = total
        row_copies.append(
            share("row", me_r, rows, row_in.at[me_r, h], s_row, r_row, h * (rows - 1))
        )

    for copy in carry_copies:
        copy.wait_recv()
    a, b, quad = amplitudes(
        [carry_in[k, 0:1, :] for k in range(cols)],
        [carry_in[k, 1:2, :] for k in range(cols)],
        phi,
        side_gain,
        width,
        me_c,
    )
    for k in range(cols):
        quad = quad + carry_in[k, 2:3, :]
    quad_in[me_r] = sum(quad[:, e : e + 128] for e in range(0, extent, 128))
    quad_copies = share("row", me_r, rows, quad_in.at[me_r], s_quad, r_quad)
    high, low = split(field + a * side_down[...] + b * side_up[...])
    for unit in range(2):
        at = slice(256 * unit, 256 * unit + 256)
        multiply(
            sums[2 * unit],
            unit,
            (high[at], low[at]),
            (row_sines_ref[0], row_sines_ref[1]),
            transpose=True,
        )

    inner = jnp.zeros((part, 128), f32)
    for h in range(HALVES):
        for copy in row_copies[h]:
            copy.wait_recv()
        at = slice(h * part, (h + 1) * part)
        a, b, quad = amplitudes(
            [row_in[k, h, :part] for k in range(rows)],
            [row_in[k, h, part:] for k in range(rows)],
            theta[at],
            gain[at],
            extent,
            me_r,
        )
        inner = inner + quad
        amp_ref[0, at] = a
        amp_ref[1, at] = b
        for first in range(h * part * 128, (h + 1) * part * 128, 256):
            lanes = slice(first, first + 256)
            t = first // 128
            a_row = jnp.concatenate([amp_ref[0, t + i : t + i + 1, :] for i in range(2)], axis=1)
            b_row = jnp.concatenate([amp_ref[1, t + i : t + i + 1, :] for i in range(2)], axis=1)
            high, low = split(a_row * down[:, lanes] + b_row * up[:, lanes])
            for unit in range(2):
                at = slice(256 * unit, 256 * unit + 256)
                multiply(
                    sums[2 * unit],
                    unit,
                    (table[0, at, lanes], table[1, at, lanes]),
                    (high, low),
                    transpose=True,
                )
    for unit in range(2):
        out_ref[:, 256 * unit : 256 * unit + 256] = pltpu.matmul_pop(sums[2 * unit])

    for copy in quad_copies:
        copy.wait_recv()
    inner = jnp.sum(inner, axis=0, keepdims=True)
    for k in range(rows):
        inner = inner + quad_in[k]
    ratio = jnp.sum(inner, axis=1, keepdims=True) / scalars_ref[1:2, 0:1]
    ratio_ref[...] = jnp.broadcast_to(ratio, ratio_ref.shape)
    for copies in (*col_copies, carry_copies, *row_copies, quad_copies):
        for copy in copies:
            copy.wait_send()


def body(rows, cols, residual, direction, ground_shift, previous):
    extent, width = residual.shape
    length = width * cols
    f32, bf16 = jnp.float32, jnp.bfloat16
    ready = 4 * length * length <= 1 << 24
    constants = tables(extent, width, cols, ready)
    vmem = pl.BlockSpec(memory_space=pltpu.VMEM)
    smem = pl.BlockSpec(memory_space=pltpu.SMEM)
    hbm = pl.BlockSpec(memory_space=pltpu.HBM)
    dma = pltpu.SemaphoreType.DMA
    per_row, per_col = max(rows - 1, 1), max(cols - 1, 1)
    operands = (residual, *constants)
    scalars = jnp.broadcast_to(jnp.stack([ground_shift, previous]), (2, 128))
    tiles = length // 128
    part = tiles // HALVES
    scratch = [pltpu.VMEM(x.shape, x.dtype) for x in operands[:6]] + [
        dma((len(operands) + length // min(512, length),)),
        pltpu.VMEM((tiles, 128), f32),
        pltpu.VMEM((2, width, length), bf16),
        pltpu.VMEM((extent, length), f32),
        pltpu.VMEM((extent, length), f32),
        pltpu.VMEM((width, extent), f32),
        pltpu.VMEM((width, extent), f32),
        pltpu.VMEM((2, tiles, 128), f32),
        pltpu.VMEM((cols, HALVES, 2 * part, 128), f32),
        pltpu.VMEM((cols, 4, extent), f32),
        pltpu.VMEM((rows, HALVES, 2 * part, 128), f32),
        pltpu.VMEM((rows, 1, 128), f32),
        dma((HALVES * per_col,)),
        dma((HALVES * per_col,)),
        dma((per_col,)),
        dma((per_col,)),
        dma((HALVES * per_row,)),
        dma((HALVES * per_row,)),
        dma((per_row,)),
        dma((per_row,)),
    ]
    if not ready:
        scratch += [
            pltpu.VMEM((2, width // 64, length), f32),
            pltpu.VMEM((4, 8, length), f32),
            pltpu.VMEM((width // 8, length), f32),
            pltpu.VMEM((width // 8, length), f32),
        ]
    held = sum(
        math.prod(ref.shape) * jnp.dtype(ref.dtype).itemsize
        for ref in scratch
        if ref.memory_space == pltpu.VMEM
    )
    solved, ratio = pl.pallas_call(
        functools.partial(kernel, rows, cols, ready),
        out_shape=(
            jax.ShapeDtypeStruct((extent, width), f32),
            jax.ShapeDtypeStruct((1, 128), f32),
        ),
        in_specs=[hbm] * len(operands) + [vmem],
        out_specs=(vmem, vmem),
        scratch_shapes=scratch,
        compiler_params=pltpu.CompilerParams(
            collective_id=0,
            has_side_effects=True,
            vmem_limit_bytes=min(held + (held >> 2) + (8 << 20), 61 << 20),
        ),
    )(*(pltpu.with_memory_space_constraint(x, pltpu.HBM) for x in operands), scalars)
    return pl.pallas_call(
        update,
        out_shape=(
            jax.ShapeDtypeStruct((extent, width), f32),
            jax.ShapeDtypeStruct((1,), f32),
        ),
        in_specs=[vmem, vmem, vmem],
        out_specs=(vmem, smem),
        compiler_params=pltpu.CompilerParams(vmem_limit_bytes=8 << 20),
    )(solved, direction, ratio)


def update(solved_ref, direction_ref, ratio_in, out_ref, ratio_out):
    ratio = ratio_in[0:1, 0:1]
    out_ref[...] = solved_ref[...] + ratio * direction_ref[...]
    ratio_out[0] = ratio_in[0, 0]


def solution(mesh):
    return jax.shard_map(
        functools.partial(body, mesh.shape["row"], mesh.shape["col"]),
        mesh=mesh,
        in_specs=(P("row", "col"), P("row", "col"), P(), P()),
        out_specs=(P("row", "col"), P()),
        check_vma=False,
    )
```

```python
import functools
import math

import jax
import jax.numpy as jnp
import numpy as np
from jax import lax
from jax.experimental import pallas as pl
from jax.experimental.pallas import tpu as pltpu
from jax.sharding import PartitionSpec as P

MESH = pl.DeviceIdType.MESH
PARTS = 2


def halves_of(table):
    high = table.astype(jnp.bfloat16)
    low = (table - high.astype(np.float64)).astype(jnp.bfloat16)
    return np.stack([high, low])


def sine_table(extent):
    index = np.arange(1, extent + 1, dtype=np.int64)
    turns = index[:, None] * index[None, :] % (2 * (extent + 1))
    table = math.sqrt(2.0 / (extent + 1)) * np.sin(np.pi * turns / (extent + 1))
    eigen = 4.0 * np.sin(np.pi * index / (2 * (extent + 1))) ** 2
    return halves_of(table), eigen


def column_cosines(width, cols):
    length = width * cols
    modes = np.arange(length, dtype=np.int64)[None, :]
    odd = 2 * np.arange(length, dtype=np.int64)[:, None] + 1
    scale = np.where(modes == 0, math.sqrt(1.0 / length), math.sqrt(2.0 / length))
    table = scale * np.cos(np.pi * (modes * odd % (4 * length)) / (2 * length))
    return halves_of(table).reshape(2, cols, width, length).swapaxes(0, 1)


def tables(extent, width, cols, ready):
    length = width * cols
    modes = np.arange(length, dtype=np.int64)[None, :]
    coarse = 64 * np.arange(length // 64, dtype=np.int64)[:, None]
    middle = 8 * np.arange(8, dtype=np.int64)[:, None]
    fine = 2 * np.arange(8, dtype=np.int64)[:, None] + 1
    coarse = np.pi * (modes * coarse % (2 * length)) / length
    middle = np.pi * (modes * middle % (2 * length)) / length
    fine = np.pi * (modes * fine % (4 * length)) / (2 * length)
    scale = np.where(modes == 0, math.sqrt(1.0 / length), math.sqrt(2.0 / length))
    far = np.stack([np.cos(coarse), np.sin(coarse)]).astype(np.float32)
    near = np.stack(
        [np.cos(middle), np.sin(middle), scale * np.cos(fine), scale * np.sin(fine)]
    ).astype(np.float32)
    waves = 4.0 * np.sin(np.pi * modes / (2 * length)) ** 2
    row_sines, row_eigen = sine_table(extent)
    col_sines, col_eigen = sine_table(width)
    both = (col_eigen[:, None] + row_eigen[None, :]).astype(np.float32)
    sources = (column_cosines(width, cols),) if ready else (far, near)
    return (
        waves.reshape(-1, 128).astype(np.float32),
        row_eigen[None, :].astype(np.float32),
        both,
        row_sines,
        col_sines,
        *sources,
    )


def split(value):
    high = value.astype(jnp.bfloat16)
    return high, (value - high.astype(jnp.float32)).astype(jnp.bfloat16)


def decay(alpha):
    h = 0.5 * jnp.sqrt(alpha)
    z = h / (1.0 + jnp.sqrt(1.0 + h * h))
    z2 = z * z
    series = jnp.full_like(z, 1.0 / 23)
    for p in range(21, 0, -2):
        series = series * z2 + 1.0 / p
    return 4.0 * z * series, 0.5 / jnp.sqrt(alpha * (1.0 + 0.25 * alpha))


def waves(ps, qs, chunk, whole):
    count = len(ps)
    fronts, backs = [], [None] * count
    left, right = jnp.zeros_like(chunk), jnp.zeros_like(chunk)
    for k in range(count):
        fronts.append(left)
        left = chunk * left + qs[k]
        backs[count - 1 - k] = right
        right = chunk * right + ps[count - 1 - k]
    images = 1.0 / (1.0 - whole * whole)
    entry = (right + whole * left) * images
    exit_ = (left + whole * right) * images
    for k in range(count):
        fronts[k] = fronts[k] + entry
        backs[count - 1 - k] = backs[count - 1 - k] + exit_
        entry, exit_ = entry * chunk, exit_ * chunk
    return fronts, backs


def amplitudes(ps, qs, theta, gain, extent, me):
    count = len(ps)
    fronts, backs = waves(
        ps, qs, jnp.exp(-theta * float(extent)), jnp.exp(-theta * float(extent * count))
    )
    far = jnp.exp(-theta * float(extent + 1))
    inside = gain / (1.0 - far * far)
    outside = gain * jnp.exp(theta)
    total = jnp.zeros_like(theta)
    mine_a, mine_b = jnp.zeros_like(theta), jnp.zeros_like(theta)
    for k in range(count):
        a = outside * fronts[k] + inside * (ps[k] - far * qs[k])
        b = outside * backs[k] + inside * (qs[k] - far * ps[k])
        total = total + a * ps[k] + b * qs[k]
        mine_a = jnp.where(me == k, a, mine_a)
        mine_b = jnp.where(me == k, b, mine_b)
    return mine_a, mine_b, total


def fill_decays(theta, lanes, down_ref, up_ref):
    blocks = down_ref.shape[0] // 8
    wide = (8, theta.shape[1])
    place = lax.broadcasted_iota(jnp.int32, wide, 0).astype(jnp.float32)
    step = jnp.exp(jnp.broadcast_to(-8.0 * theta, wide))
    down = jnp.exp(-theta * (place + 1.0))
    up = jnp.exp(-theta * (8.0 - place))
    for n in range(blocks):
        down_ref[8 * n : 8 * n + 8, lanes] = down
        up_ref[8 * (blocks - 1 - n) : 8 * (blocks - n), lanes] = up
        down, up = down * step, up * step


def edge_sums(value, theta):
    wide = (8, theta.shape[1])
    place = lax.broadcasted_iota(jnp.int32, wide, 0).astype(jnp.float32)
    step = jnp.exp(jnp.broadcast_to(-8.0 * theta, wide))
    blocks = [value[i : i + 8] for i in range(0, value.shape[0], 8)]
    up, down = blocks[0], blocks[-1]
    for n in range(1, len(blocks)):
        up = up * step + blocks[n]
        down = down * step + blocks[-1 - n]
    return (
        jnp.sum(down * jnp.exp(-theta * (place + 1.0)), axis=0, keepdims=True),
        jnp.sum(up * jnp.exp(-theta * (8.0 - place)), axis=0, keepdims=True),
    )


def fill_all(theta_ref, down_ref, up_ref):
    blocks = down_ref.shape[0] // 8
    tiles = theta_ref.shape[0]
    place = lax.broadcasted_iota(jnp.int32, (8, 128), 0).astype(jnp.float32)
    for first in range(0, tiles, 8):
        group = range(first, min(first + 8, tiles))
        thetas = [theta_ref[t : t + 1, :] for t in group]
        steps = [jnp.exp(jnp.broadcast_to(-8.0 * theta, (8, 128))) for theta in thetas]
        down = [jnp.exp(-theta * (place + 1.0)) for theta in thetas]
        up = [jnp.exp(-theta * (8.0 - place)) for theta in thetas]

        def step(n, carry):
            down, up = carry
            top = pl.ds(pl.multiple_of(8 * n, 8), 8)
            bottom = pl.ds(pl.multiple_of(8 * (blocks - 1 - n), 8), 8)
            for i, t in enumerate(group):
                down_ref[top, t * 128 : (t + 1) * 128] = down[i]
                up_ref[bottom, t * 128 : (t + 1) * 128] = up[i]
            return (
                [d * s for d, s in zip(down, steps)],
                [u * s for u, s in zip(up, steps)],
            )

        lax.fori_loop(0, blocks, step, (down, up))


def kernel(rows, cols, ready, *refs):
    def run(*sums):
        apply(rows, cols, ready, sums, *refs)

    extent = refs[0].shape[0]
    pl.run_scoped(run, *(pltpu.ACC(m)((extent, 256), jnp.float32) for m in (0, 0, 1, 1)))


def multiply(total, unit, right, left, transpose=False):
    high, low = left
    pltpu.matmul_push_rhs(right[0], 0, unit, transpose=transpose)
    pltpu.matmul_acc_lhs(total, high, load_staged_rhs=0)
    pltpu.matmul_acc_lhs(total, low)
    pltpu.matmul_push_rhs(right[1], 1, unit, transpose=transpose)
    pltpu.matmul_acc_lhs(total, high, load_staged_rhs=1)


def apply(rows, cols, ready, sums, *refs):
    sources = 1 if ready else 2
    residual_hbm, waves_hbm, row_eigen_hbm, both_hbm, row_sines_hbm, col_sines_hbm = refs[:6]
    source_hbms = refs[6 : 6 + sources]
    scalars_ref, out_ref, ratio_ref = refs[6 + sources : 9 + sources]
    residual_ref, waves_ref, row_eigen_ref, both_ref, row_sines_ref, col_sines_ref = refs[
        9 + sources : 15 + sources
    ]
    (
        load_sems,
        theta_ref,
        table,
        down,
        up,
        side_down,
        side_up,
        amp_ref,
        col_in,
        carry_in,
        row_in,
        quad_in,
        block_in,
        s_col,
        r_col,
        s_carry,
        r_carry,
        s_row,
        r_row,
        s_quad,
        r_quad,
        s_block,
        r_block,
        *spare,
    ) = refs[15 + sources :]
    me_r = lax.axis_index("row")
    me_c = lax.axis_index("col")
    extent, width = residual_ref.shape
    length = table.shape[2]
    tiles = length // 128
    part = tiles // PARTS
    f32 = jnp.float32

    barrier = pltpu.get_barrier_semaphore()
    for o in range(1, cols):
        pl.semaphore_signal(
            barrier, inc=1, device_id={"col": lax.rem(me_c + o, cols)}, device_id_type=MESH
        )
    for o in range(1, rows):
        pl.semaphore_signal(
            barrier, inc=1, device_id={"row": lax.rem(me_r + o, rows)}, device_id_type=MESH
        )

    loads = []

    def load(source, landing):
        copy = pltpu.make_async_copy(source, landing, load_sems.at[len(loads)])
        copy.start()
        loads.append(copy)
        return copy

    waves_load = load(waves_hbm, waves_ref)
    residual_load = load(residual_hbm, residual_ref)
    chunk = min(512, length)
    table_loads = []
    if ready:
        for first in range(0, length, chunk):
            lanes = slice(first, first + chunk)
            table_loads.append(load(source_hbms[0].at[me_c, :, :, lanes], table.at[:, :, lanes]))
    else:
        far_ref, near_ref, cos_ref, sin_ref = spare
        per = width // 64
        own = source_hbms[0].at[:, pl.ds(pl.multiple_of(me_c * per, per), per), :]
        far_load = load(own, far_ref)
        near_load = load(source_hbms[1], near_ref)
    late_loads = [
        load(source, landing)
        for source, landing in (
            (row_eigen_hbm, row_eigen_ref),
            (row_sines_hbm, row_sines_ref),
            (col_sines_hbm, col_sines_ref),
            (both_hbm, both_ref),
        )
    ]

    def share(axis, me, count, ref, send_sems, recv_sems, first=0):
        copies = []
        for o in range(1, count):
            copy = pltpu.make_async_remote_copy(
                src_ref=ref,
                dst_ref=ref,
                send_sem=send_sems.at[first + o - 1],
                recv_sem=recv_sems.at[first + o - 1],
                device_id={axis: lax.rem(me + o, count)},
                device_id_type=MESH,
            )
            copy.start()
            copies.append(copy)
        return copies

    shift = scalars_ref[0:1, 0:1]
    waves_load.wait()
    theta, gain = decay(waves_ref[...] + shift)
    theta_ref[...] = theta

    if not ready:
        far_load.wait()
        near_load.wait()
        for u in range(per):
            rows_u = slice(8 * u, 8 * u + 8)
            cos_u, sin_u = far_ref[0, u : u + 1, :], far_ref[1, u : u + 1, :]
            cos_ref[rows_u, :] = cos_u * near_ref[0] - sin_u * near_ref[1]
            sin_ref[rows_u, :] = sin_u * near_ref[0] + cos_u * near_ref[1]

        span = min(1024, length)

        def fill(n, carry):
            at = pl.ds(pl.multiple_of(16 * n, 16), 16)
            for first in range(0, length, span):
                lanes = slice(first, first + span)
                pieces = []
                for k in range(2):
                    row = pl.ds(2 * n + k, 1)
                    pieces.append(
                        cos_ref[row, lanes] * near_ref[2, :, lanes]
                        - sin_ref[row, lanes] * near_ref[3, :, lanes]
                    )
                high, low = split(jnp.concatenate(pieces, axis=0))
                table[0, at, lanes] = high
                table[1, at, lanes] = low
            return carry

        lax.fori_loop(0, width // 16, fill, 0)

    col_copies = []
    for h in range(PARTS):
        if ready:
            for first in range(0, length, chunk):
                if h == first * PARTS // length:
                    table_loads[first // chunk].wait()
        if h == 0:
            residual_load.wait()
            r_hi, r_lo = split(residual_ref[...])
        for tile in range(h * part // 2, (h + 1) * part // 2):
            lanes = slice(256 * tile, 256 * tile + 256)
            unit = tile % 2
            total = sums[2 * unit + tile // 2 % 2]
            for first in range(0, width, 256):
                at = slice(first, first + 256)
                multiply(
                    total,
                    unit,
                    (table[0, at, lanes], table[1, at, lanes]),
                    (r_hi[:, at], r_lo[:, at]),
                )
            value = pltpu.matmul_pop(total)
            p, q = edge_sums(
                value, jnp.concatenate([theta_ref[2 * tile + i : 2 * tile + i + 1] for i in (0, 1)], axis=1)
            )
            for i in range(2):
                at = 2 * tile + i - h * part
                piece = slice(128 * i, 128 * i + 128)
                col_in[me_c, h, at : at + 1, :] = p[:, piece]
                col_in[me_c, h, part + at : part + at + 1, :] = q[:, piece]
        if h == 0:
            pl.semaphore_wait(barrier, rows + cols - 2)
        col_copies.append(
            share("col", me_c, cols, col_in.at[me_c, h], s_col, r_col, h * (cols - 1))
        )

    for copy in late_loads:
        copy.wait()
    turned_hi, turned_lo = split(residual_ref[...].T)
    tops = [slice(256 * unit, 256 * unit + 256) for unit in range(2)]
    for unit in range(2):
        multiply(
            sums[2 * unit],
            unit,
            (row_sines_ref[0], row_sines_ref[1]),
            (turned_hi[tops[unit]], turned_lo[tops[unit]]),
        )
    modal = jnp.concatenate([pltpu.matmul_pop(sums[2 * unit]) for unit in range(2)], axis=0)
    phi, side_gain = decay(row_eigen_ref[...] + shift)
    fill_decays(phi, slice(0, extent), side_down, side_up)
    carry_in[me_c, 0:1, :] = jnp.sum(modal * side_down[...], axis=0, keepdims=True)
    carry_in[me_c, 1:2, :] = jnp.sum(modal * side_up[...], axis=0, keepdims=True)
    carry_copies = share("col", me_c, cols, carry_in.at[me_c], s_carry, r_carry)

    def across(value):
        high, low = split(value)
        for unit in range(2):
            for at in tops:
                multiply(
                    sums[2 * unit],
                    unit,
                    (high[at], low[at]),
                    (col_sines_ref[0, tops[unit], at], col_sines_ref[1, tops[unit], at]),
                )
        return jnp.concatenate([pltpu.matmul_pop(sums[2 * unit]) for unit in range(2)], axis=0)

    spectrum = across(modal)
    scaled = spectrum / (both_ref[...] + shift)
    block = jnp.sum(spectrum * scaled, axis=0, keepdims=True)
    block_in[me_c] = sum(block[:, e : e + 128] for e in range(0, extent, 128))
    block_copies = share("col", me_c, cols, block_in.at[me_c], s_block, r_block)
    field = across(scaled)
    fill_all(theta_ref, down, up)

    row_copies = []
    for h in range(PARTS):
        for copy in col_copies[h]:
            copy.wait_recv()
        total = col_in[0, h]
        for k in range(1, cols):
            total = total + col_in[k, h]
        row_in[me_r, h] = total
        row_copies.append(
            share("row", me_r, rows, row_in.at[me_r, h], s_row, r_row, h * (rows - 1))
        )

    for copy in carry_copies:
        copy.wait_recv()
    a, b, quad = amplitudes(
        [carry_in[k, 0:1, :] for k in range(cols)],
        [carry_in[k, 1:2, :] for k in range(cols)],
        phi,
        side_gain,
        width,
        me_c,
    )
    quad = sum(quad[:, e : e + 128] for e in range(0, extent, 128))
    high, low = split(field + a * side_down[...] + b * side_up[...])
    for unit in range(2):
        at = slice(256 * unit, 256 * unit + 256)
        multiply(
            sums[2 * unit],
            unit,
            (high[at], low[at]),
            (row_sines_ref[0], row_sines_ref[1]),
            transpose=True,
        )
    for copy in block_copies:
        copy.wait_recv()
    for k in range(cols):
        quad = quad + block_in[k]
    quad_in[me_r] = quad
    quad_copies = share("row", me_r, rows, quad_in.at[me_r], s_quad, r_quad)

    inner = jnp.zeros((part, 128), f32)
    for h in range(PARTS):
        for copy in row_copies[h]:
            copy.wait_recv()
        at = slice(h * part, (h + 1) * part)
        a, b, quad = amplitudes(
            [row_in[k, h, :part] for k in range(rows)],
            [row_in[k, h, part:] for k in range(rows)],
            theta[at],
            gain[at],
            extent,
            me_r,
        )
        inner = inner + quad
        amp_ref[0, at] = a
        amp_ref[1, at] = b
        for first in range(h * part * 128, (h + 1) * part * 128, 256):
            lanes = slice(first, first + 256)
            if first == length - 256:
                for copy in quad_copies:
                    copy.wait_recv()
                inner = jnp.sum(inner, axis=0, keepdims=True)
                for k in range(rows):
                    inner = inner + quad_in[k]
                ratio = jnp.sum(inner, axis=1, keepdims=True) / scalars_ref[1:2, 0:1]
                ratio_ref[...] = jnp.broadcast_to(ratio, ratio_ref.shape)
            t = first // 128
            a_row = jnp.concatenate([amp_ref[0, t + i : t + i + 1, :] for i in range(2)], axis=1)
            b_row = jnp.concatenate([amp_ref[1, t + i : t + i + 1, :] for i in range(2)], axis=1)
            high, low = split(a_row * down[:, lanes] + b_row * up[:, lanes])
            for unit in range(2):
                at = slice(256 * unit, 256 * unit + 256)
                multiply(
                    sums[2 * unit],
                    unit,
                    (table[0, at, lanes], table[1, at, lanes]),
                    (high, low),
                    transpose=True,
                )
    for unit in range(2):
        out_ref[:, 256 * unit : 256 * unit + 256] = pltpu.matmul_pop(sums[2 * unit])
    for copies in (*col_copies, carry_copies, block_copies, *row_copies, quad_copies):
        for copy in copies:
            copy.wait_send()


def body(rows, cols, residual, direction, ground_shift, previous):
    extent, width = residual.shape
    length = width * cols
    f32, bf16 = jnp.float32, jnp.bfloat16
    ready = 4 * length * length <= 1 << 24
    constants = tables(extent, width, cols, ready)
    vmem = pl.BlockSpec(memory_space=pltpu.VMEM)
    smem = pl.BlockSpec(memory_space=pltpu.SMEM)
    hbm = pl.BlockSpec(memory_space=pltpu.HBM)
    dma = pltpu.SemaphoreType.DMA
    per_row, per_col = max(rows - 1, 1), max(cols - 1, 1)
    operands = (residual, *constants)
    scalars = jnp.broadcast_to(jnp.stack([ground_shift, previous]), (2, 128))
    tiles = length // 128
    part = tiles // PARTS
    scratch = [pltpu.VMEM(x.shape, x.dtype) for x in operands[:6]] + [
        dma((len(operands) + length // min(512, length),)),
        pltpu.VMEM((tiles, 128), f32),
        pltpu.VMEM((2, width, length), bf16),
        pltpu.VMEM((extent, length), f32),
        pltpu.VMEM((extent, length), f32),
        pltpu.VMEM((width, extent), f32),
        pltpu.VMEM((width, extent), f32),
        pltpu.VMEM((2, tiles, 128), f32),
        pltpu.VMEM((cols, PARTS, 2 * part, 128), f32),
        pltpu.VMEM((cols, 2, extent), f32),
        pltpu.VMEM((rows, PARTS, 2 * part, 128), f32),
        pltpu.VMEM((rows, 1, 128), f32),
        pltpu.VMEM((cols, 1, 128), f32),
        dma((PARTS * per_col,)),
        dma((PARTS * per_col,)),
        dma((per_col,)),
        dma((per_col,)),
        dma((PARTS * per_row,)),
        dma((PARTS * per_row,)),
        dma((per_row,)),
        dma((per_row,)),
        dma((per_col,)),
        dma((per_col,)),
    ]
    if not ready:
        scratch += [
            pltpu.VMEM((2, width // 64, length), f32),
            pltpu.VMEM((4, 8, length), f32),
            pltpu.VMEM((width // 8, length), f32),
            pltpu.VMEM((width // 8, length), f32),
        ]
    held = sum(
        math.prod(ref.shape) * jnp.dtype(ref.dtype).itemsize
        for ref in scratch
        if ref.memory_space == pltpu.VMEM
    )
    solved, ratio = pl.pallas_call(
        functools.partial(kernel, rows, cols, ready),
        out_shape=(
            jax.ShapeDtypeStruct((extent, width), f32),
            jax.ShapeDtypeStruct((1, 128), f32),
        ),
        in_specs=[hbm] * len(operands) + [vmem],
        out_specs=(vmem, vmem),
        scratch_shapes=scratch,
        compiler_params=pltpu.CompilerParams(
            collective_id=0,
            has_side_effects=True,
            vmem_limit_bytes=min(held + (held >> 2) + (8 << 20), 61 << 20),
        ),
    )(*(pltpu.with_memory_space_constraint(x, pltpu.HBM) for x in operands), scalars)
    return pl.pallas_call(
        update,
        out_shape=(
            jax.ShapeDtypeStruct((extent, width), f32),
            jax.ShapeDtypeStruct((1,), f32),
        ),
        in_specs=[vmem, vmem, vmem],
        out_specs=(vmem, smem),
        compiler_params=pltpu.CompilerParams(vmem_limit_bytes=8 << 20),
    )(solved, direction, ratio)


def update(solved_ref, direction_ref, ratio_in, out_ref, ratio_out):
    ratio = ratio_in[0:1, 0:1]
    out_ref[...] = solved_ref[...] + ratio * direction_ref[...]
    ratio_out[0] = ratio_in[0, 0]


def solution(mesh):
    return jax.shard_map(
        functools.partial(body, mesh.shape["row"], mesh.shape["col"]),
        mesh=mesh,
        in_specs=(P("row", "col"), P("row", "col"), P(), P()),
        out_specs=(P("row", "col"), P()),
        check_vma=False,
    )
```

```python
import functools
import math

import jax
import jax.numpy as jnp
import numpy as np
from jax import lax
from jax.experimental import pallas as pl
from jax.experimental.pallas import tpu as pltpu
from jax.sharding import PartitionSpec as P

MESH = pl.DeviceIdType.MESH
PARTS = 2


def halves_of(table):
    high = table.astype(jnp.bfloat16)
    low = (table - high.astype(np.float64)).astype(jnp.bfloat16)
    return np.stack([high, low])


def sine_table(extent):
    index = np.arange(1, extent + 1, dtype=np.int64)
    turns = index[:, None] * index[None, :] % (2 * (extent + 1))
    table = math.sqrt(2.0 / (extent + 1)) * np.sin(np.pi * turns / (extent + 1))
    eigen = 4.0 * np.sin(np.pi * index / (2 * (extent + 1))) ** 2
    return halves_of(table), eigen


def column_cosines(width, cols):
    length = width * cols
    modes = np.arange(length, dtype=np.int64)[None, :]
    odd = 2 * np.arange(length, dtype=np.int64)[:, None] + 1
    scale = np.where(modes == 0, math.sqrt(1.0 / length), math.sqrt(2.0 / length))
    table = scale * np.cos(np.pi * (modes * odd % (4 * length)) / (2 * length))
    return halves_of(table).reshape(2, cols, width, length).swapaxes(0, 1)


def tables(extent, width, cols, ready):
    length = width * cols
    modes = np.arange(length, dtype=np.int64)[None, :]
    coarse = 64 * np.arange(length // 64, dtype=np.int64)[:, None]
    middle = 8 * np.arange(8, dtype=np.int64)[:, None]
    fine = 2 * np.arange(8, dtype=np.int64)[:, None] + 1
    coarse = np.pi * (modes * coarse % (2 * length)) / length
    middle = np.pi * (modes * middle % (2 * length)) / length
    fine = np.pi * (modes * fine % (4 * length)) / (2 * length)
    scale = np.where(modes == 0, math.sqrt(1.0 / length), math.sqrt(2.0 / length))
    far = np.stack([np.cos(coarse), np.sin(coarse)]).astype(np.float32)
    near = np.stack(
        [np.cos(middle), np.sin(middle), scale * np.cos(fine), scale * np.sin(fine)]
    ).astype(np.float32)
    waves = 4.0 * np.sin(np.pi * modes / (2 * length)) ** 2
    row_sines, row_eigen = sine_table(extent)
    col_sines, col_eigen = sine_table(width)
    both = (col_eigen[:, None] + row_eigen[None, :]).astype(np.float32)
    sources = (column_cosines(width, cols),) if ready else (far, near)
    return (
        waves.reshape(-1, 128).astype(np.float32),
        row_eigen[None, :].astype(np.float32),
        both,
        row_sines,
        col_sines,
        *sources,
    )


def split(value):
    high = value.astype(jnp.bfloat16)
    return high, (value - high.astype(jnp.float32)).astype(jnp.bfloat16)


def decay(alpha):
    h = 0.5 * jnp.sqrt(alpha)
    z = h / (1.0 + jnp.sqrt(1.0 + h * h))
    z2 = z * z
    series = jnp.full_like(z, 1.0 / 23)
    for p in range(21, 0, -2):
        series = series * z2 + 1.0 / p
    return 4.0 * z * series, 0.5 / jnp.sqrt(alpha * (1.0 + 0.25 * alpha))


def waves(ps, qs, chunk, whole):
    count = len(ps)
    fronts, backs = [], [None] * count
    left, right = jnp.zeros_like(chunk), jnp.zeros_like(chunk)
    for k in range(count):
        fronts.append(left)
        left = chunk * left + qs[k]
        backs[count - 1 - k] = right
        right = chunk * right + ps[count - 1 - k]
    images = 1.0 / (1.0 - whole * whole)
    entry = (right + whole * left) * images
    exit_ = (left + whole * right) * images
    for k in range(count):
        fronts[k] = fronts[k] + entry
        backs[count - 1 - k] = backs[count - 1 - k] + exit_
        entry, exit_ = entry * chunk, exit_ * chunk
    return fronts, backs


def amplitudes(ps, qs, theta, gain, extent, me):
    count = len(ps)
    fronts, backs = waves(
        ps, qs, jnp.exp(-theta * float(extent)), jnp.exp(-theta * float(extent * count))
    )
    far = jnp.exp(-theta * float(extent + 1))
    inside = gain / (1.0 - far * far)
    outside = gain * jnp.exp(theta)
    total = jnp.zeros_like(theta)
    mine_a, mine_b = jnp.zeros_like(theta), jnp.zeros_like(theta)
    for k in range(count):
        a = outside * fronts[k] + inside * (ps[k] - far * qs[k])
        b = outside * backs[k] + inside * (qs[k] - far * ps[k])
        total = total + a * ps[k] + b * qs[k]
        mine_a = jnp.where(me == k, a, mine_a)
        mine_b = jnp.where(me == k, b, mine_b)
    return mine_a, mine_b, total


def fill_decays(theta, lanes, down_ref, up_ref):
    blocks = down_ref.shape[0] // 8
    wide = (8, theta.shape[1])
    place = lax.broadcasted_iota(jnp.int32, wide, 0).astype(jnp.float32)
    step = jnp.exp(jnp.broadcast_to(-8.0 * theta, wide))
    down = jnp.exp(-theta * (place + 1.0))
    up = jnp.exp(-theta * (8.0 - place))
    for n in range(blocks):
        down_ref[8 * n : 8 * n + 8, lanes] = down
        up_ref[8 * (blocks - 1 - n) : 8 * (blocks - n), lanes] = up
        down, up = down * step, up * step


def edge_sums(value, theta):
    wide = (8, theta.shape[1])
    place = lax.broadcasted_iota(jnp.int32, wide, 0).astype(jnp.float32)
    step = jnp.exp(jnp.broadcast_to(-8.0 * theta, wide))
    blocks = [value[i : i + 8] for i in range(0, value.shape[0], 8)]
    up, down = blocks[0], blocks[-1]
    for n in range(1, len(blocks)):
        up = up * step + blocks[n]
        down = down * step + blocks[-1 - n]
    return (
        jnp.sum(down * jnp.exp(-theta * (place + 1.0)), axis=0, keepdims=True),
        jnp.sum(up * jnp.exp(-theta * (8.0 - place)), axis=0, keepdims=True),
    )


def fill_all(theta_ref, down_ref, up_ref):
    blocks = down_ref.shape[0] // 8
    tiles = theta_ref.shape[0]
    place = lax.broadcasted_iota(jnp.int32, (8, 128), 0).astype(jnp.float32)
    for first in range(0, tiles, 8):
        group = range(first, min(first + 8, tiles))
        thetas = [theta_ref[t : t + 1, :] for t in group]
        steps = [jnp.exp(jnp.broadcast_to(-8.0 * theta, (8, 128))) for theta in thetas]
        down = [jnp.exp(-theta * (place + 1.0)) for theta in thetas]
        up = [jnp.exp(-theta * (8.0 - place)) for theta in thetas]

        def step(n, carry):
            down, up = carry
            top = pl.ds(pl.multiple_of(8 * n, 8), 8)
            bottom = pl.ds(pl.multiple_of(8 * (blocks - 1 - n), 8), 8)
            for i, t in enumerate(group):
                down_ref[top, t * 128 : (t + 1) * 128] = down[i]
                up_ref[bottom, t * 128 : (t + 1) * 128] = up[i]
            return (
                [d * s for d, s in zip(down, steps)],
                [u * s for u, s in zip(up, steps)],
            )

        lax.fori_loop(0, blocks, step, (down, up))


def kernel(rows, cols, ready, *refs):
    def run(*sums):
        apply(rows, cols, ready, sums, *refs)

    extent = refs[0].shape[0]
    pl.run_scoped(run, *(pltpu.ACC(m)((extent, 256), jnp.float32) for m in (0, 0, 1, 1)))


def multiply(total, unit, right, left, transpose=False):
    high, low = left
    pltpu.matmul_push_rhs(right[0], 0, unit, transpose=transpose)
    pltpu.matmul_acc_lhs(total, high, load_staged_rhs=0)
    pltpu.matmul_acc_lhs(total, low)
    pltpu.matmul_push_rhs(right[1], 1, unit, transpose=transpose)
    pltpu.matmul_acc_lhs(total, high, load_staged_rhs=1)


def apply(rows, cols, ready, sums, *refs):
    sources = 1 if ready else 2
    residual_hbm, waves_hbm, row_eigen_hbm, both_hbm, row_sines_hbm, col_sines_hbm = refs[:6]
    source_hbms = refs[6 : 6 + sources]
    scalars_ref, out_ref, ratio_ref = refs[6 + sources : 9 + sources]
    residual_ref, waves_ref, row_eigen_ref, both_ref, row_sines_ref, col_sines_ref = refs[
        9 + sources : 15 + sources
    ]
    (
        load_sems,
        theta_ref,
        table,
        down,
        up,
        side_down,
        side_up,
        amp_ref,
        col_in,
        carry_in,
        row_in,
        quad_in,
        block_in,
        s_col,
        r_col,
        s_carry,
        r_carry,
        s_row,
        r_row,
        s_quad,
        r_quad,
        s_block,
        r_block,
        *spare,
    ) = refs[15 + sources :]
    me_r = lax.axis_index("row")
    me_c = lax.axis_index("col")
    extent, width = residual_ref.shape
    length = table.shape[2]
    tiles = length // 128
    part = tiles // PARTS
    f32 = jnp.float32

    barrier = pltpu.get_barrier_semaphore()
    for o in range(1, cols):
        pl.semaphore_signal(
            barrier, inc=1, device_id={"col": lax.rem(me_c + o, cols)}, device_id_type=MESH
        )
    for o in range(1, rows):
        pl.semaphore_signal(
            barrier, inc=1, device_id={"row": lax.rem(me_r + o, rows)}, device_id_type=MESH
        )

    loads = []

    def load(source, landing):
        copy = pltpu.make_async_copy(source, landing, load_sems.at[len(loads)])
        copy.start()
        loads.append(copy)
        return copy

    waves_load = load(waves_hbm, waves_ref)
    residual_load = load(residual_hbm, residual_ref)
    early_loads = [load(row_eigen_hbm, row_eigen_ref), load(row_sines_hbm, row_sines_ref)]
    chunk = min(512, length)
    table_loads = []
    if ready:
        for first in range(0, length, chunk):
            lanes = slice(first, first + chunk)
            table_loads.append(load(source_hbms[0].at[me_c, :, :, lanes], table.at[:, :, lanes]))
    else:
        far_ref, near_ref, cos_ref, sin_ref = spare
        per = width // 64
        own = source_hbms[0].at[:, pl.ds(pl.multiple_of(me_c * per, per), per), :]
        far_load = load(own, far_ref)
        near_load = load(source_hbms[1], near_ref)
    late_loads = [
        load(source, landing)
        for source, landing in (
            (col_sines_hbm, col_sines_ref),
            (both_hbm, both_ref),
        )
    ]

    def share(axis, me, count, ref, send_sems, recv_sems, first=0):
        copies = []
        for o in range(1, count):
            copy = pltpu.make_async_remote_copy(
                src_ref=ref,
                dst_ref=ref,
                send_sem=send_sems.at[first + o - 1],
                recv_sem=recv_sems.at[first + o - 1],
                device_id={axis: lax.rem(me + o, count)},
                device_id_type=MESH,
            )
            copy.start()
            copies.append(copy)
        return copies

    shift = scalars_ref[0:1, 0:1]
    waves_load.wait()
    theta, gain = decay(waves_ref[...] + shift)
    theta_ref[...] = theta

    if not ready:
        far_load.wait()
        near_load.wait()
        for u in range(per):
            rows_u = slice(8 * u, 8 * u + 8)
            cos_u, sin_u = far_ref[0, u : u + 1, :], far_ref[1, u : u + 1, :]
            cos_ref[rows_u, :] = cos_u * near_ref[0] - sin_u * near_ref[1]
            sin_ref[rows_u, :] = sin_u * near_ref[0] + cos_u * near_ref[1]

        span = min(1024, length)

        def fill(n, carry):
            at = pl.ds(pl.multiple_of(16 * n, 16), 16)
            for first in range(0, length, span):
                lanes = slice(first, first + span)
                pieces = []
                for k in range(2):
                    row = pl.ds(2 * n + k, 1)
                    pieces.append(
                        cos_ref[row, lanes] * near_ref[2, :, lanes]
                        - sin_ref[row, lanes] * near_ref[3, :, lanes]
                    )
                high, low = split(jnp.concatenate(pieces, axis=0))
                table[0, at, lanes] = high
                table[1, at, lanes] = low
            return carry

        lax.fori_loop(0, width // 16, fill, 0)

    residual_load.wait()
    for copy in early_loads:
        copy.wait()
    r_hi, r_lo = split(residual_ref[...])
    turned_hi, turned_lo = split(residual_ref[...].T)
    tops = [slice(256 * unit, 256 * unit + 256) for unit in range(2)]
    for unit in range(2):
        multiply(
            sums[2 * unit],
            unit,
            (row_sines_ref[0], row_sines_ref[1]),
            (turned_hi[tops[unit]], turned_lo[tops[unit]]),
        )
    modal = jnp.concatenate([pltpu.matmul_pop(sums[2 * unit]) for unit in range(2)], axis=0)
    phi, side_gain = decay(row_eigen_ref[...] + shift)
    fill_decays(phi, slice(0, extent), side_down, side_up)
    carry_in[me_c, 0:1, :] = jnp.sum(modal * side_down[...], axis=0, keepdims=True)
    carry_in[me_c, 1:2, :] = jnp.sum(modal * side_up[...], axis=0, keepdims=True)

    col_copies = []
    for h in range(PARTS):
        if ready:
            for first in range(0, length, chunk):
                if h == first * PARTS // length:
                    table_loads[first // chunk].wait()
        for tile in range(h * part // 2, (h + 1) * part // 2):
            lanes = slice(256 * tile, 256 * tile + 256)
            unit = tile % 2
            total = sums[2 * unit + tile // 2 % 2]
            for first in range(0, width, 256):
                at = slice(first, first + 256)
                multiply(
                    total,
                    unit,
                    (table[0, at, lanes], table[1, at, lanes]),
                    (r_hi[:, at], r_lo[:, at]),
                )
            value = pltpu.matmul_pop(total)
            p, q = edge_sums(
                value, jnp.concatenate([theta_ref[2 * tile + i : 2 * tile + i + 1] for i in (0, 1)], axis=1)
            )
            for i in range(2):
                at = 2 * tile + i - h * part
                piece = slice(128 * i, 128 * i + 128)
                col_in[me_c, h, at : at + 1, :] = p[:, piece]
                col_in[me_c, h, part + at : part + at + 1, :] = q[:, piece]
        if h == 0:
            pl.semaphore_wait(barrier, rows + cols - 2)
        col_copies.append(
            share("col", me_c, cols, col_in.at[me_c, h], s_col, r_col, h * (cols - 1))
        )
        if h == 0:
            carry_copies = share("col", me_c, cols, carry_in.at[me_c], s_carry, r_carry)

    for copy in late_loads:
        copy.wait()

    def across(value):
        high, low = split(value)
        for unit in range(2):
            for at in tops:
                multiply(
                    sums[2 * unit],
                    unit,
                    (high[at], low[at]),
                    (col_sines_ref[0, tops[unit], at], col_sines_ref[1, tops[unit], at]),
                )
        return jnp.concatenate([pltpu.matmul_pop(sums[2 * unit]) for unit in range(2)], axis=0)

    spectrum = across(modal)
    scaled = spectrum / (both_ref[...] + shift)
    block = jnp.sum(spectrum * scaled, axis=0, keepdims=True)
    block_in[me_c] = sum(block[:, e : e + 128] for e in range(0, extent, 128))
    block_copies = share("col", me_c, cols, block_in.at[me_c], s_block, r_block)
    field = across(scaled)
    fill_all(theta_ref, down, up)

    row_copies = []
    for h in range(PARTS):
        for copy in col_copies[h]:
            copy.wait_recv()
        total = col_in[0, h]
        for k in range(1, cols):
            total = total + col_in[k, h]
        row_in[me_r, h] = total
        row_copies.append(
            share("row", me_r, rows, row_in.at[me_r, h], s_row, r_row, h * (rows - 1))
        )

    for copy in carry_copies:
        copy.wait_recv()
    a, b, quad = amplitudes(
        [carry_in[k, 0:1, :] for k in range(cols)],
        [carry_in[k, 1:2, :] for k in range(cols)],
        phi,
        side_gain,
        width,
        me_c,
    )
    quad = sum(quad[:, e : e + 128] for e in range(0, extent, 128))
    high, low = split(field + a * side_down[...] + b * side_up[...])
    for unit in range(2):
        at = slice(256 * unit, 256 * unit + 256)
        multiply(
            sums[2 * unit],
            unit,
            (high[at], low[at]),
            (row_sines_ref[0], row_sines_ref[1]),
            transpose=True,
        )
    for copy in block_copies:
        copy.wait_recv()
    for k in range(cols):
        quad = quad + block_in[k]
    quad_in[me_r] = quad
    quad_copies = share("row", me_r, rows, quad_in.at[me_r], s_quad, r_quad)

    inner = jnp.zeros((part, 128), f32)
    for h in range(PARTS):
        for copy in row_copies[h]:
            copy.wait_recv()
        at = slice(h * part, (h + 1) * part)
        a, b, quad = amplitudes(
            [row_in[k, h, :part] for k in range(rows)],
            [row_in[k, h, part:] for k in range(rows)],
            theta[at],
            gain[at],
            extent,
            me_r,
        )
        inner = inner + quad
        amp_ref[0, at] = a
        amp_ref[1, at] = b
        for first in range(h * part * 128, (h + 1) * part * 128, 256):
            lanes = slice(first, first + 256)
            if first == length - 256:
                for copy in quad_copies:
                    copy.wait_recv()
                inner = jnp.sum(inner, axis=0, keepdims=True)
                for k in range(rows):
                    inner = inner + quad_in[k]
                ratio = jnp.sum(inner, axis=1, keepdims=True) / scalars_ref[1:2, 0:1]
                ratio_ref[...] = jnp.broadcast_to(ratio, ratio_ref.shape)
            t = first // 128
            a_row = jnp.concatenate([amp_ref[0, t + i : t + i + 1, :] for i in range(2)], axis=1)
            b_row = jnp.concatenate([amp_ref[1, t + i : t + i + 1, :] for i in range(2)], axis=1)
            high, low = split(a_row * down[:, lanes] + b_row * up[:, lanes])
            for unit in range(2):
                at = slice(256 * unit, 256 * unit + 256)
                multiply(
                    sums[2 * unit],
                    unit,
                    (table[0, at, lanes], table[1, at, lanes]),
                    (high, low),
                    transpose=True,
                )
    for unit in range(2):
        out_ref[:, 256 * unit : 256 * unit + 256] = pltpu.matmul_pop(sums[2 * unit])
    for copies in (*col_copies, carry_copies, block_copies, *row_copies, quad_copies):
        for copy in copies:
            copy.wait_send()


def body(rows, cols, residual, direction, ground_shift, previous):
    extent, width = residual.shape
    length = width * cols
    f32, bf16 = jnp.float32, jnp.bfloat16
    ready = 4 * length * length <= 1 << 24
    constants = tables(extent, width, cols, ready)
    vmem = pl.BlockSpec(memory_space=pltpu.VMEM)
    smem = pl.BlockSpec(memory_space=pltpu.SMEM)
    hbm = pl.BlockSpec(memory_space=pltpu.HBM)
    dma = pltpu.SemaphoreType.DMA
    per_row, per_col = max(rows - 1, 1), max(cols - 1, 1)
    operands = (residual, *constants)
    scalars = jnp.broadcast_to(jnp.stack([ground_shift, previous]), (2, 128))
    tiles = length // 128
    part = tiles // PARTS
    scratch = [pltpu.VMEM(x.shape, x.dtype) for x in operands[:6]] + [
        dma((len(operands) + length // min(512, length),)),
        pltpu.VMEM((tiles, 128), f32),
        pltpu.VMEM((2, width, length), bf16),
        pltpu.VMEM((extent, length), f32),
        pltpu.VMEM((extent, length), f32),
        pltpu.VMEM((width, extent), f32),
        pltpu.VMEM((width, extent), f32),
        pltpu.VMEM((2, tiles, 128), f32),
        pltpu.VMEM((cols, PARTS, 2 * part, 128), f32),
        pltpu.VMEM((cols, 2, extent), f32),
        pltpu.VMEM((rows, PARTS, 2 * part, 128), f32),
        pltpu.VMEM((rows, 1, 128), f32),
        pltpu.VMEM((cols, 1, 128), f32),
        dma((PARTS * per_col,)),
        dma((PARTS * per_col,)),
        dma((per_col,)),
        dma((per_col,)),
        dma((PARTS * per_row,)),
        dma((PARTS * per_row,)),
        dma((per_row,)),
        dma((per_row,)),
        dma((per_col,)),
        dma((per_col,)),
    ]
    if not ready:
        scratch += [
            pltpu.VMEM((2, width // 64, length), f32),
            pltpu.VMEM((4, 8, length), f32),
            pltpu.VMEM((width // 8, length), f32),
            pltpu.VMEM((width // 8, length), f32),
        ]
    held = sum(
        math.prod(ref.shape) * jnp.dtype(ref.dtype).itemsize
        for ref in scratch
        if ref.memory_space == pltpu.VMEM
    )
    solved, ratio = pl.pallas_call(
        functools.partial(kernel, rows, cols, ready),
        out_shape=(
            jax.ShapeDtypeStruct((extent, width), f32),
            jax.ShapeDtypeStruct((1, 128), f32),
        ),
        in_specs=[hbm] * len(operands) + [vmem],
        out_specs=(vmem, vmem),
        scratch_shapes=scratch,
        compiler_params=pltpu.CompilerParams(
            collective_id=0,
            has_side_effects=True,
            vmem_limit_bytes=min(held + (held >> 2) + (8 << 20), 61 << 20),
        ),
    )(*(pltpu.with_memory_space_constraint(x, pltpu.HBM) for x in operands), scalars)
    return pl.pallas_call(
        update,
        out_shape=(
            jax.ShapeDtypeStruct((extent, width), f32),
            jax.ShapeDtypeStruct((1,), f32),
        ),
        in_specs=[vmem, vmem, vmem],
        out_specs=(vmem, smem),
        compiler_params=pltpu.CompilerParams(vmem_limit_bytes=8 << 20),
    )(solved, direction, ratio)


def update(solved_ref, direction_ref, ratio_in, out_ref, ratio_out):
    ratio = ratio_in[0:1, 0:1]
    out_ref[...] = solved_ref[...] + ratio * direction_ref[...]
    ratio_out[0] = ratio_in[0, 0]


def solution(mesh):
    return jax.shard_map(
        functools.partial(body, mesh.shape["row"], mesh.shape["col"]),
        mesh=mesh,
        in_specs=(P("row", "col"), P("row", "col"), P(), P()),
        out_specs=(P("row", "col"), P()),
        check_vma=False,
    )
```

```python
import functools
import math

import jax
import jax.numpy as jnp
import numpy as np
from jax import lax
from jax.experimental import pallas as pl
from jax.experimental.pallas import tpu as pltpu
from jax.sharding import PartitionSpec as P

MESH = pl.DeviceIdType.MESH
PARTS = 2


def halves_of(table):
    high = table.astype(jnp.bfloat16)
    low = (table - high.astype(np.float64)).astype(jnp.bfloat16)
    return np.stack([high, low])


def sine_table(extent):
    index = np.arange(1, extent + 1, dtype=np.int64)
    turns = index[:, None] * index[None, :] % (2 * (extent + 1))
    table = math.sqrt(2.0 / (extent + 1)) * np.sin(np.pi * turns / (extent + 1))
    eigen = 4.0 * np.sin(np.pi * index / (2 * (extent + 1))) ** 2
    return halves_of(table), eigen


def column_cosines(width, cols):
    length = width * cols
    modes = np.arange(length, dtype=np.int64)[None, :]
    odd = 2 * np.arange(length, dtype=np.int64)[:, None] + 1
    scale = np.where(modes == 0, math.sqrt(1.0 / length), math.sqrt(2.0 / length))
    table = scale * np.cos(np.pi * (modes * odd % (4 * length)) / (2 * length))
    return halves_of(table).reshape(2, cols, width, length).swapaxes(0, 1)


def tables(extent, width, cols, ready):
    length = width * cols
    modes = np.arange(length, dtype=np.int64)[None, :]
    coarse = 64 * np.arange(length // 64, dtype=np.int64)[:, None]
    middle = 8 * np.arange(8, dtype=np.int64)[:, None]
    fine = 2 * np.arange(8, dtype=np.int64)[:, None] + 1
    coarse = np.pi * (modes * coarse % (2 * length)) / length
    middle = np.pi * (modes * middle % (2 * length)) / length
    fine = np.pi * (modes * fine % (4 * length)) / (2 * length)
    scale = np.where(modes == 0, math.sqrt(1.0 / length), math.sqrt(2.0 / length))
    far = np.stack([np.cos(coarse), np.sin(coarse)]).astype(np.float32)
    near = np.stack(
        [np.cos(middle), np.sin(middle), scale * np.cos(fine), scale * np.sin(fine)]
    ).astype(np.float32)
    waves = 4.0 * np.sin(np.pi * modes / (2 * length)) ** 2
    row_sines, row_eigen = sine_table(extent)
    col_sines, col_eigen = sine_table(width)
    both = (col_eigen[:, None] + row_eigen[None, :]).astype(np.float32)
    sources = (column_cosines(width, cols),) if ready else (far, near)
    return (
        waves.reshape(-1, 128).astype(np.float32),
        row_eigen[None, :].astype(np.float32),
        both,
        row_sines,
        col_sines,
        *sources,
    )


def split(value):
    high = value.astype(jnp.bfloat16)
    return high, (value - high.astype(jnp.float32)).astype(jnp.bfloat16)


def decay(alpha):
    h = 0.5 * jnp.sqrt(alpha)
    z = h / (1.0 + jnp.sqrt(1.0 + h * h))
    z2 = z * z
    series = jnp.full_like(z, 1.0 / 23)
    for p in range(21, 0, -2):
        series = series * z2 + 1.0 / p
    return 4.0 * z * series, 0.5 / jnp.sqrt(alpha * (1.0 + 0.25 * alpha))


def waves(ps, qs, chunk, whole):
    count = len(ps)
    fronts, backs = [], [None] * count
    left, right = jnp.zeros_like(chunk), jnp.zeros_like(chunk)
    for k in range(count):
        fronts.append(left)
        left = chunk * left + qs[k]
        backs[count - 1 - k] = right
        right = chunk * right + ps[count - 1 - k]
    images = 1.0 / (1.0 - whole * whole)
    entry = (right + whole * left) * images
    exit_ = (left + whole * right) * images
    for k in range(count):
        fronts[k] = fronts[k] + entry
        backs[count - 1 - k] = backs[count - 1 - k] + exit_
        entry, exit_ = entry * chunk, exit_ * chunk
    return fronts, backs


def amplitudes(ps, qs, theta, gain, extent, me):
    count = len(ps)
    fronts, backs = waves(
        ps, qs, jnp.exp(-theta * float(extent)), jnp.exp(-theta * float(extent * count))
    )
    far = jnp.exp(-theta * float(extent + 1))
    inside = gain / (1.0 - far * far)
    outside = gain * jnp.exp(theta)
    total = jnp.zeros_like(theta)
    mine_a, mine_b = jnp.zeros_like(theta), jnp.zeros_like(theta)
    for k in range(count):
        a = outside * fronts[k] + inside * (ps[k] - far * qs[k])
        b = outside * backs[k] + inside * (qs[k] - far * ps[k])
        total = total + a * ps[k] + b * qs[k]
        mine_a = jnp.where(me == k, a, mine_a)
        mine_b = jnp.where(me == k, b, mine_b)
    return mine_a, mine_b, total


def fill_decays(theta, lanes, down_ref, up_ref):
    blocks = down_ref.shape[0] // 8
    wide = (8, theta.shape[1])
    place = lax.broadcasted_iota(jnp.int32, wide, 0).astype(jnp.float32)
    step = jnp.exp(jnp.broadcast_to(-8.0 * theta, wide))
    down = jnp.exp(-theta * (place + 1.0))
    up = jnp.exp(-theta * (8.0 - place))
    for n in range(blocks):
        down_ref[8 * n : 8 * n + 8, lanes] = down
        up_ref[8 * (blocks - 1 - n) : 8 * (blocks - n), lanes] = up
        down, up = down * step, up * step


def edge_sums(value, theta):
    wide = (8, theta.shape[1])
    place = lax.broadcasted_iota(jnp.int32, wide, 0).astype(jnp.float32)
    step = jnp.exp(jnp.broadcast_to(-8.0 * theta, wide))
    blocks = [value[i : i + 8] for i in range(0, value.shape[0], 8)]
    up, down = blocks[0], blocks[-1]
    for n in range(1, len(blocks)):
        up = up * step + blocks[n]
        down = down * step + blocks[-1 - n]
    return (
        jnp.sum(down * jnp.exp(-theta * (place + 1.0)), axis=0, keepdims=True),
        jnp.sum(up * jnp.exp(-theta * (8.0 - place)), axis=0, keepdims=True),
    )


def fill_all(theta_ref, down_ref, up_ref):
    blocks = down_ref.shape[0] // 8
    tiles = theta_ref.shape[0]
    place = lax.broadcasted_iota(jnp.int32, (8, 128), 0).astype(jnp.float32)
    for first in range(0, tiles, 8):
        group = range(first, min(first + 8, tiles))
        thetas = [theta_ref[t : t + 1, :] for t in group]
        steps = [jnp.exp(jnp.broadcast_to(-8.0 * theta, (8, 128))) for theta in thetas]
        down = [jnp.exp(-theta * (place + 1.0)) for theta in thetas]
        up = [jnp.exp(-theta * (8.0 - place)) for theta in thetas]

        def step(n, carry):
            down, up = carry
            top = pl.ds(pl.multiple_of(8 * n, 8), 8)
            bottom = pl.ds(pl.multiple_of(8 * (blocks - 1 - n), 8), 8)
            for i, t in enumerate(group):
                down_ref[top, t * 128 : (t + 1) * 128] = down[i]
                up_ref[bottom, t * 128 : (t + 1) * 128] = up[i]
            return (
                [d * s for d, s in zip(down, steps)],
                [u * s for u, s in zip(up, steps)],
            )

        lax.fori_loop(0, blocks, step, (down, up))


def kernel(rows, cols, ready, *refs):
    def run(*sums):
        apply(rows, cols, ready, sums, *refs)

    extent = refs[0].shape[0]
    pl.run_scoped(run, *(pltpu.ACC(m)((extent, 256), jnp.float32) for m in (0, 0, 1, 1)))


def multiply(total, unit, right, left, transpose=False):
    high, low = left
    pltpu.matmul_push_rhs(right[0], 0, unit, transpose=transpose)
    pltpu.matmul_acc_lhs(total, high, load_staged_rhs=0)
    pltpu.matmul_acc_lhs(total, low)
    pltpu.matmul_push_rhs(right[1], 1, unit, transpose=transpose)
    pltpu.matmul_acc_lhs(total, high, load_staged_rhs=1)


def apply(rows, cols, ready, sums, *refs):
    sources = 1 if ready else 2
    residual_hbm, waves_hbm, row_eigen_hbm, both_hbm, row_sines_hbm, col_sines_hbm = refs[:6]
    source_hbms = refs[6 : 6 + sources]
    shift_ref, previous_ref, out_ref, ratio_ref = refs[6 + sources : 10 + sources]
    residual_ref, waves_ref, row_eigen_ref, both_ref, row_sines_ref, col_sines_ref = refs[
        10 + sources : 16 + sources
    ]
    (
        load_sems,
        theta_ref,
        table,
        down,
        up,
        side_down,
        side_up,
        amp_ref,
        col_in,
        carry_in,
        row_in,
        quad_in,
        block_in,
        s_col,
        r_col,
        s_carry,
        r_carry,
        s_row,
        r_row,
        s_quad,
        r_quad,
        s_block,
        r_block,
        *spare,
    ) = refs[16 + sources :]
    me_r = lax.axis_index("row")
    me_c = lax.axis_index("col")
    extent, width = residual_ref.shape
    length = table.shape[2]
    tiles = length // 128
    part = tiles // PARTS
    f32 = jnp.float32

    barrier = pltpu.get_barrier_semaphore()
    for o in range(1, cols):
        pl.semaphore_signal(
            barrier, inc=1, device_id={"col": lax.rem(me_c + o, cols)}, device_id_type=MESH
        )
    for o in range(1, rows):
        pl.semaphore_signal(
            barrier, inc=1, device_id={"row": lax.rem(me_r + o, rows)}, device_id_type=MESH
        )

    loads = []

    def load(source, landing):
        copy = pltpu.make_async_copy(source, landing, load_sems.at[len(loads)])
        copy.start()
        loads.append(copy)
        return copy

    waves_load = load(waves_hbm, waves_ref)
    residual_load = load(residual_hbm, residual_ref)
    early_loads = [load(row_eigen_hbm, row_eigen_ref), load(row_sines_hbm, row_sines_ref)]
    chunk = min(512, length)
    table_loads = []
    if ready:
        for first in range(0, length, chunk):
            lanes = slice(first, first + chunk)
            table_loads.append(load(source_hbms[0].at[me_c, :, :, lanes], table.at[:, :, lanes]))
    else:
        far_ref, near_ref, cos_ref, sin_ref = spare
        per = width // 64
        own = source_hbms[0].at[:, pl.ds(pl.multiple_of(me_c * per, per), per), :]
        far_load = load(own, far_ref)
        near_load = load(source_hbms[1], near_ref)
    late_loads = [
        load(source, landing)
        for source, landing in (
            (col_sines_hbm, col_sines_ref),
            (both_hbm, both_ref),
        )
    ]

    def share(axis, me, count, ref, send_sems, recv_sems, first=0):
        copies = []
        for o in range(1, count):
            copy = pltpu.make_async_remote_copy(
                src_ref=ref,
                dst_ref=ref,
                send_sem=send_sems.at[first + o - 1],
                recv_sem=recv_sems.at[first + o - 1],
                device_id={axis: lax.rem(me + o, count)},
                device_id_type=MESH,
            )
            copy.start()
            copies.append(copy)
        return copies

    shift = shift_ref[0]
    waves_load.wait()
    theta, gain = decay(waves_ref[...] + shift)
    theta_ref[...] = theta

    if not ready:
        far_load.wait()
        near_load.wait()
        for u in range(per):
            rows_u = slice(8 * u, 8 * u + 8)
            cos_u, sin_u = far_ref[0, u : u + 1, :], far_ref[1, u : u + 1, :]
            cos_ref[rows_u, :] = cos_u * near_ref[0] - sin_u * near_ref[1]
            sin_ref[rows_u, :] = sin_u * near_ref[0] + cos_u * near_ref[1]

        span = min(1024, length)

        def fill(n, carry):
            at = pl.ds(pl.multiple_of(16 * n, 16), 16)
            for first in range(0, length, span):
                lanes = slice(first, first + span)
                pieces = []
                for k in range(2):
                    row = pl.ds(2 * n + k, 1)
                    pieces.append(
                        cos_ref[row, lanes] * near_ref[2, :, lanes]
                        - sin_ref[row, lanes] * near_ref[3, :, lanes]
                    )
                high, low = split(jnp.concatenate(pieces, axis=0))
                table[0, at, lanes] = high
                table[1, at, lanes] = low
            return carry

        lax.fori_loop(0, width // 16, fill, 0)

    residual_load.wait()
    for copy in early_loads:
        copy.wait()
    r_hi, r_lo = split(residual_ref[...])
    turned_hi, turned_lo = split(residual_ref[...].T)
    tops = [slice(256 * unit, 256 * unit + 256) for unit in range(2)]
    for unit in range(2):
        multiply(
            sums[2 * unit],
            unit,
            (row_sines_ref[0], row_sines_ref[1]),
            (turned_hi[tops[unit]], turned_lo[tops[unit]]),
        )
    modal = jnp.concatenate([pltpu.matmul_pop(sums[2 * unit]) for unit in range(2)], axis=0)
    phi, side_gain = decay(row_eigen_ref[...] + shift)
    fill_decays(phi, slice(0, extent), side_down, side_up)
    carry_in[me_c, 0:1, :] = jnp.sum(modal * side_down[...], axis=0, keepdims=True)
    carry_in[me_c, 1:2, :] = jnp.sum(modal * side_up[...], axis=0, keepdims=True)

    col_copies = []
    for h in range(PARTS):
        if ready:
            for first in range(0, length, chunk):
                if h == first * PARTS // length:
                    table_loads[first // chunk].wait()
        for tile in range(h * part // 2, (h + 1) * part // 2):
            lanes = slice(256 * tile, 256 * tile + 256)
            unit = tile % 2
            total = sums[2 * unit + tile // 2 % 2]
            for first in range(0, width, 256):
                at = slice(first, first + 256)
                multiply(
                    total,
                    unit,
                    (table[0, at, lanes], table[1, at, lanes]),
                    (r_hi[:, at], r_lo[:, at]),
                )
            value = pltpu.matmul_pop(total)
            p, q = edge_sums(
                value, jnp.concatenate([theta_ref[2 * tile + i : 2 * tile + i + 1] for i in (0, 1)], axis=1)
            )
            for i in range(2):
                at = 2 * tile + i - h * part
                piece = slice(128 * i, 128 * i + 128)
                col_in[me_c, h, at : at + 1, :] = p[:, piece]
                col_in[me_c, h, part + at : part + at + 1, :] = q[:, piece]
        if h == 0:
            pl.semaphore_wait(barrier, rows + cols - 2)
        col_copies.append(
            share("col", me_c, cols, col_in.at[me_c, h], s_col, r_col, h * (cols - 1))
        )
        if h == 0:
            carry_copies = share("col", me_c, cols, carry_in.at[me_c], s_carry, r_carry)

    for copy in late_loads:
        copy.wait()

    def across(value):
        high, low = split(value)
        for unit in range(2):
            for at in tops:
                multiply(
                    sums[2 * unit],
                    unit,
                    (high[at], low[at]),
                    (col_sines_ref[0, tops[unit], at], col_sines_ref[1, tops[unit], at]),
                )
        return jnp.concatenate([pltpu.matmul_pop(sums[2 * unit]) for unit in range(2)], axis=0)

    spectrum = across(modal)
    scaled = spectrum / (both_ref[...] + shift)
    block = jnp.sum(spectrum * scaled, axis=0, keepdims=True)
    block_in[me_c] = sum(block[:, e : e + 128] for e in range(0, extent, 128))
    block_copies = share("col", me_c, cols, block_in.at[me_c], s_block, r_block)
    field = across(scaled)
    fill_all(theta_ref, down, up)

    row_copies = []
    for h in range(PARTS):
        for copy in col_copies[h]:
            copy.wait_recv()
        total = col_in[0, h]
        for k in range(1, cols):
            total = total + col_in[k, h]
        row_in[me_r, h] = total
        row_copies.append(
            share("row", me_r, rows, row_in.at[me_r, h], s_row, r_row, h * (rows - 1))
        )

    for copy in carry_copies:
        copy.wait_recv()
    a, b, quad = amplitudes(
        [carry_in[k, 0:1, :] for k in range(cols)],
        [carry_in[k, 1:2, :] for k in range(cols)],
        phi,
        side_gain,
        width,
        me_c,
    )
    quad = sum(quad[:, e : e + 128] for e in range(0, extent, 128))
    high, low = split(field + a * side_down[...] + b * side_up[...])
    for unit in range(2):
        at = slice(256 * unit, 256 * unit + 256)
        multiply(
            sums[2 * unit],
            unit,
            (high[at], low[at]),
            (row_sines_ref[0], row_sines_ref[1]),
            transpose=True,
        )
    for copy in block_copies:
        copy.wait_recv()
    for k in range(cols):
        quad = quad + block_in[k]
    quad_in[me_r] = quad
    quad_copies = share("row", me_r, rows, quad_in.at[me_r], s_quad, r_quad)

    inner = jnp.zeros((part, 128), f32)
    for h in range(PARTS):
        for copy in row_copies[h]:
            copy.wait_recv()
        at = slice(h * part, (h + 1) * part)
        a, b, quad = amplitudes(
            [row_in[k, h, :part] for k in range(rows)],
            [row_in[k, h, part:] for k in range(rows)],
            theta[at],
            gain[at],
            extent,
            me_r,
        )
        inner = inner + quad
        amp_ref[0, at] = a
        amp_ref[1, at] = b
        for first in range(h * part * 128, (h + 1) * part * 128, 256):
            lanes = slice(first, first + 256)
            if first == length - 256:
                for copy in quad_copies:
                    copy.wait_recv()
                inner = jnp.sum(inner, axis=0, keepdims=True)
                for k in range(rows):
                    inner = inner + quad_in[k]
                ratio = jnp.sum(inner, axis=1, keepdims=True) / previous_ref[0]
                ratio_ref[...] = jnp.broadcast_to(ratio, ratio_ref.shape)
            t = first // 128
            a_row = jnp.concatenate([amp_ref[0, t + i : t + i + 1, :] for i in range(2)], axis=1)
            b_row = jnp.concatenate([amp_ref[1, t + i : t + i + 1, :] for i in range(2)], axis=1)
            high, low = split(a_row * down[:, lanes] + b_row * up[:, lanes])
            for unit in range(2):
                at = slice(256 * unit, 256 * unit + 256)
                multiply(
                    sums[2 * unit],
                    unit,
                    (table[0, at, lanes], table[1, at, lanes]),
                    (high, low),
                    transpose=True,
                )
    for unit in range(2):
        out_ref[:, 256 * unit : 256 * unit + 256] = pltpu.matmul_pop(sums[2 * unit])
    for copies in (*col_copies, carry_copies, block_copies, *row_copies, quad_copies):
        for copy in copies:
            copy.wait_send()


def body(rows, cols, residual, direction, ground_shift, previous):
    extent, width = residual.shape
    length = width * cols
    f32, bf16 = jnp.float32, jnp.bfloat16
    ready = 4 * length * length <= 1 << 24
    constants = tables(extent, width, cols, ready)
    vmem = pl.BlockSpec(memory_space=pltpu.VMEM)
    smem = pl.BlockSpec(memory_space=pltpu.SMEM)
    hbm = pl.BlockSpec(memory_space=pltpu.HBM)
    dma = pltpu.SemaphoreType.DMA
    per_row, per_col = max(rows - 1, 1), max(cols - 1, 1)
    operands = (residual, *constants)
    tiles = length // 128
    part = tiles // PARTS
    scratch = [pltpu.VMEM(x.shape, x.dtype) for x in operands[:6]] + [
        dma((len(operands) + length // min(512, length),)),
        pltpu.VMEM((tiles, 128), f32),
        pltpu.VMEM((2, width, length), bf16),
        pltpu.VMEM((extent, length), f32),
        pltpu.VMEM((extent, length), f32),
        pltpu.VMEM((width, extent), f32),
        pltpu.VMEM((width, extent), f32),
        pltpu.VMEM((2, tiles, 128), f32),
        pltpu.VMEM((cols, PARTS, 2 * part, 128), f32),
        pltpu.VMEM((cols, 2, extent), f32),
        pltpu.VMEM((rows, PARTS, 2 * part, 128), f32),
        pltpu.VMEM((rows, 1, 128), f32),
        pltpu.VMEM((cols, 1, 128), f32),
        dma((PARTS * per_col,)),
        dma((PARTS * per_col,)),
        dma((per_col,)),
        dma((per_col,)),
        dma((PARTS * per_row,)),
        dma((PARTS * per_row,)),
        dma((per_row,)),
        dma((per_row,)),
        dma((per_col,)),
        dma((per_col,)),
    ]
    if not ready:
        scratch += [
            pltpu.VMEM((2, width // 64, length), f32),
            pltpu.VMEM((4, 8, length), f32),
            pltpu.VMEM((width // 8, length), f32),
            pltpu.VMEM((width // 8, length), f32),
        ]
    held = sum(
        math.prod(ref.shape) * jnp.dtype(ref.dtype).itemsize
        for ref in scratch
        if ref.memory_space == pltpu.VMEM
    )
    solved, ratio = pl.pallas_call(
        functools.partial(kernel, rows, cols, ready),
        out_shape=(
            jax.ShapeDtypeStruct((extent, width), f32),
            jax.ShapeDtypeStruct((1, 128), f32),
        ),
        in_specs=[hbm] * len(operands) + [smem, smem],
        out_specs=(vmem, vmem),
        scratch_shapes=scratch,
        compiler_params=pltpu.CompilerParams(
            collective_id=0,
            has_side_effects=True,
            vmem_limit_bytes=min(held + (held >> 2) + (8 << 20), 61 << 20),
        ),
    )(*(pltpu.with_memory_space_constraint(x, pltpu.HBM) for x in operands), ground_shift, previous)
    return pl.pallas_call(
        update,
        out_shape=(
            jax.ShapeDtypeStruct((extent, width), f32),
            jax.ShapeDtypeStruct((1,), f32),
        ),
        in_specs=[vmem, vmem, vmem],
        out_specs=(vmem, smem),
        compiler_params=pltpu.CompilerParams(vmem_limit_bytes=8 << 20),
    )(solved, direction, ratio)


def update(solved_ref, direction_ref, ratio_in, out_ref, ratio_out):
    ratio = ratio_in[0:1, 0:1]
    out_ref[...] = solved_ref[...] + ratio * direction_ref[...]
    ratio_out[0] = ratio_in[0, 0]


def solution(mesh):
    return jax.shard_map(
        functools.partial(body, mesh.shape["row"], mesh.shape["col"]),
        mesh=mesh,
        in_specs=(P("row", "col"), P("row", "col"), P(), P()),
        out_specs=(P("row", "col"), P()),
        check_vma=False,
    )
```
